32 devices in a mesh: dp: 4 (over z), ep: 8 (over y, x, core).
Axes of the slice: x: 2, y: 2, z: 4, core: 2. Of those that a mesh axis runs over, the one named last changes fastest.
Arguments:
- tok_x: bfloat16 [16384, 4096], P(('dp', 'ep'))
- tok_dy: bfloat16 [16384, 4096], P(('dp', 'ep'))
- exp_first: int32 [16384], P(('dp', 'ep'))
- exp_second: int32 [16384], P(('dp', 'ep'))
- eligible: int32 [16384, 8], P(('dp', 'ep'))
- slot_first: int32 [16384], P(('dp', 'ep'))
- slot_second: int32 [16384], P(('dp', 'ep'))
- ln_weight: bfloat16 [4096], replicated
- ln_bias: bfloat16 [4096], replicated
- router: bfloat16 [4096, 8], replicated
- w_gate: bfloat16 [8, 4096, 1376], P('ep')
- w_up: bfloat16 [8, 4096, 1376], P('ep')
- w_down: bfloat16 [8, 1376, 4096], P('ep')
Outputs:
- output 1: bfloat16 [16384, 4096], P(('dp', 'ep'))
- output 2: bfloat16 [16384, 4096], P(('dp', 'ep'))
- output 3: float32 [8, 4096, 1376], P('ep')
- output 4: float32 [8, 4096, 1376], P('ep')
- output 5: float32 [8, 1376, 4096], P('ep')
- output 6: float32 [4096, 8], replicated
- output 7: float32 [4096], replicated
- output 8: float32 [4096], replicated
All inputs are finite; a program needn't handle non-finite values.
Results may differ from the reference program's by a relative error of at most 0.00494142.
Values are sent between devices in bfloat16 or wider.
A program may use at most 1 GiB of HBM per device.

```python
import jax
import jax.numpy as jnp
from jax import lax

SHARDS = 32
TOK_DEV = 512
D_MODEL = 4096
FF_DIM = 1376
EXPERTS = 8
SLOT_CAP = 192
LN_EPS = 1e-5


def draw_routing(rng_key):
    n_tok = SHARDS * TOK_DEV
    key_list = jax.random.split(rng_key, 5)
    pick_a = jax.random.randint(key_list[0], (n_tok,), 0, EXPERTS)
    pick_b = jax.random.randint(key_list[1], (n_tok,), 0, EXPERTS)
    pick_c = jax.random.randint(key_list[2], (n_tok,), 0, EXPERTS)
    first_pick = jnp.minimum(jnp.minimum(pick_a, pick_b), pick_c)
    second_pick = (first_pick + 1 + jax.random.randint(key_list[3], (n_tok,), 0, EXPERTS - 1)) % EXPERTS
    expert_ids = jnp.arange(EXPERTS)
    hot_first = (first_pick[:, None] == expert_ids[None, :]).astype(jnp.int32)
    hot_second = (second_pick[:, None] == expert_ids[None, :]).astype(jnp.int32)
    extra_bits = (jax.random.randint(key_list[4], (n_tok, EXPERTS), 0, 8) == 0).astype(jnp.int32)
    eligible = jnp.maximum(extra_bits, jnp.maximum(hot_first, hot_second))
    per_first = hot_first.reshape(SHARDS, TOK_DEV, EXPERTS)
    per_second = hot_second.reshape(SHARDS, TOK_DEV, EXPERTS)
    rank_first = jnp.sum((jnp.cumsum(per_first, axis=1) - per_first) * per_first, axis=2).reshape(n_tok)
    used_first = jnp.sum(per_first, axis=1, keepdims=True)
    rank_second = jnp.sum((jnp.cumsum(per_second, axis=1) - per_second + used_first) * per_second, axis=2).reshape(n_tok)
    slot_first = jnp.where(rank_first < SLOT_CAP, rank_first, -1)
    slot_second = jnp.where(rank_second < SLOT_CAP, rank_second, -1)
    return first_pick, second_pick, eligible, slot_first, slot_second


def setup_inputs(seed: int = 0) -> dict:
    key_list = jax.random.split(jax.random.key(seed), 10)
    n_tok = SHARDS * TOK_DEV
    first_pick, second_pick, eligible, slot_first, slot_second = draw_routing(key_list[0])
    tok_x = jax.random.normal(key_list[1], (n_tok, D_MODEL), jnp.float32).astype(jnp.bfloat16)
    tok_dy = jax.random.normal(key_list[2], (n_tok, D_MODEL), jnp.float32).astype(jnp.bfloat16)
    ln_weight = (1.0 + 0.3 * jax.random.normal(key_list[3], (D_MODEL,), jnp.float32)).astype(jnp.bfloat16)
    ln_bias = (0.3 * jax.random.normal(key_list[4], (D_MODEL,), jnp.float32)).astype(jnp.bfloat16)
    router = (1.5 * D_MODEL ** -0.5 * jax.random.normal(key_list[5], (D_MODEL, EXPERTS), jnp.float32)).astype(jnp.bfloat16)
    w_gate = (D_MODEL ** -0.5 * jax.random.normal(key_list[6], (EXPERTS, D_MODEL, FF_DIM), jnp.float32)).astype(jnp.bfloat16)
    w_up = (D_MODEL ** -0.5 * jax.random.normal(key_list[7], (EXPERTS, D_MODEL, FF_DIM), jnp.float32)).astype(jnp.bfloat16)
    w_down = (3.0 * FF_DIM ** -0.5 * jax.random.normal(key_list[8], (EXPERTS, FF_DIM, D_MODEL), jnp.float32)).astype(jnp.bfloat16)
    return {'tok_x': tok_x, 'tok_dy': tok_dy, 'exp_first': first_pick, 'exp_second': second_pick,
            'eligible': eligible, 'slot_first': slot_first, 'slot_second': slot_second,
            'ln_weight': ln_weight, 'ln_bias': ln_bias, 'router': router,
            'w_gate': w_gate, 'w_up': w_up, 'w_down': w_down}


def layer_norm(x_rows, ln_weight, ln_bias):
    x_float = x_rows.astype(jnp.float32)
    centered = x_float - jnp.mean(x_float, axis=-1, keepdims=True)
    inv_std = lax.rsqrt(jnp.mean(centered * centered, axis=-1, keepdims=True) + LN_EPS)
    x_hat = centered * inv_std
    hidden = (x_hat * ln_weight.astype(jnp.float32) + ln_bias.astype(jnp.float32)).astype(jnp.bfloat16)
    return hidden, x_hat, inv_std


def layer_norm_back(grad_h, x_hat, inv_std, ln_weight):
    scaled = grad_h * ln_weight.astype(jnp.float32)
    return inv_std * (scaled - jnp.mean(scaled, axis=-1, keepdims=True)
                      - x_hat * jnp.mean(scaled * x_hat, axis=-1, keepdims=True))


def masked_gate(logits, allowed, choice):
    expert_ids = jnp.arange(logits.shape[-1])
    prob_all = jax.nn.softmax(jnp.where(allowed, logits, -1e30), axis=-1)
    picked = (choice[:, None] == expert_ids[None, :]).astype(jnp.float32)
    return jnp.sum(prob_all * picked, axis=-1), prob_all, picked


def expert_pass(operands):
    hid_rows, grad_rows, gate_w, up_w, down_w = operands
    pre_gate = jnp.dot(hid_rows, gate_w, preferred_element_type=jnp.float32)
    pre_up = jnp.dot(hid_rows, up_w, preferred_element_type=jnp.float32)
    sig_gate = jax.nn.sigmoid(pre_gate)
    silu_gate = pre_gate * sig_gate
    inner_act = (silu_gate * pre_up).astype(jnp.bfloat16)
    exp_out = jnp.dot(inner_act, down_w, preferred_element_type=jnp.float32).astype(jnp.bfloat16)
    grad_inner = jnp.dot(grad_rows, down_w.T, preferred_element_type=jnp.float32)
    grad_pre_gate = (grad_inner * pre_up * sig_gate * (1.0 + pre_gate * (1.0 - sig_gate))).astype(jnp.bfloat16)
    grad_pre_up = (grad_inner * silu_gate).astype(jnp.bfloat16)
    grad_hid = (jnp.dot(grad_pre_gate, gate_w.T, preferred_element_type=jnp.float32)
                + jnp.dot(grad_pre_up, up_w.T, preferred_element_type=jnp.float32)).astype(jnp.bfloat16)
    dw_gate = jnp.dot(hid_rows.T, grad_pre_gate, preferred_element_type=jnp.float32)
    dw_up = jnp.dot(hid_rows.T, grad_pre_up, preferred_element_type=jnp.float32)
    dw_down = jnp.dot(inner_act.T, grad_rows, preferred_element_type=jnp.float32)
    return exp_out, grad_hid, dw_gate, dw_up, dw_down


def reference(tok_x, tok_dy, exp_first, exp_second, eligible, slot_first, slot_second,
              ln_weight, ln_bias, router, w_gate, w_up, w_down):
    n_tok = tok_x.shape[0]
    hidden, x_hat, inv_std = layer_norm(tok_x, ln_weight, ln_bias)
    logits = jnp.dot(hidden, router, preferred_element_type=jnp.float32)
    expert_ids = jnp.arange(EXPERTS)
    allowed = eligible > 0
    gate_one, prob_one, pick_one = masked_gate(logits, allowed, exp_first)
    gate_two, prob_two, pick_two = masked_gate(logits, allowed & (expert_ids[None, :] != exp_first[:, None]), exp_second)
    n_rows = EXPERTS * SHARDS * SLOT_CAP
    shard_idx = jnp.arange(n_tok) // TOK_DEV
    row_one = jnp.where(slot_first >= 0, (exp_first * SHARDS + shard_idx) * SLOT_CAP + slot_first, n_rows)
    row_two = jnp.where(slot_second >= 0, (exp_second * SHARDS + shard_idx) * SLOT_CAP + slot_second, n_rows)
    dy_float = tok_dy.astype(jnp.float32)
    grad_one = (gate_one[:, None] * dy_float).astype(jnp.bfloat16)
    grad_two = (gate_two[:, None] * dy_float).astype(jnp.bfloat16)
    empty_rows = jnp.zeros((n_rows, D_MODEL), jnp.bfloat16)
    hid_buf = empty_rows.at[row_one].set(hidden, mode='drop').at[row_two].set(hidden, mode='drop')
    grad_buf = empty_rows.at[row_one].set(grad_one, mode='drop').at[row_two].set(grad_two, mode='drop')
    exp_out, grad_hid, dw_gate, dw_up, dw_down = lax.map(
        expert_pass,
        (hid_buf.reshape(EXPERTS, SHARDS * SLOT_CAP, D_MODEL), grad_buf.reshape(EXPERTS, SHARDS * SLOT_CAP, D_MODEL),
         w_gate, w_up, w_down))
    exp_out = exp_out.reshape(n_rows, D_MODEL)
    grad_hid = grad_hid.reshape(n_rows, D_MODEL)
    out_one = jnp.take(exp_out, row_one, axis=0, mode='fill', fill_value=0).astype(jnp.float32)
    out_two = jnp.take(exp_out, row_two, axis=0, mode='fill', fill_value=0).astype(jnp.float32)
    y_mix = gate_one[:, None] * out_one + gate_two[:, None] * out_two
    out_tok = (tok_x.astype(jnp.float32) + y_mix).astype(jnp.bfloat16)
    dgate_one = jnp.sum(dy_float * out_one, axis=-1)
    dgate_two = jnp.sum(dy_float * out_two, axis=-1)
    d_logits = ((dgate_one * gate_one)[:, None] * (pick_one - prob_one)
                + (dgate_two * gate_two)[:, None] * (pick_two - prob_two)).astype(jnp.bfloat16)
    d_router = jnp.dot(hidden.T, d_logits, preferred_element_type=jnp.float32)
    grad_h = (jnp.dot(d_logits, router.T, preferred_element_type=jnp.float32)
              + jnp.take(grad_hid, row_one, axis=0, mode='fill', fill_value=0).astype(jnp.float32)
              + jnp.take(grad_hid, row_two, axis=0, mode='fill', fill_value=0).astype(jnp.float32))
    d_ln_weight = jnp.sum(grad_h * x_hat, axis=0)
    d_ln_bias = jnp.sum(grad_h, axis=0)
    dx_tok = (dy_float + layer_norm_back(grad_h, x_hat, inv_std, ln_weight)).astype(jnp.bfloat16)
    return (out_tok, dx_tok, dw_gate, dw_up, dw_down, d_router, d_ln_weight, d_ln_bias)
```

```python
import jax
import jax.numpy as jnp
from jax import lax
from jax.sharding import PartitionSpec as P

LN_EPS = 1e-5
f32 = jnp.float32
bf16 = jnp.bfloat16


def layer_norm(x_rows, ln_weight, ln_bias):
    x_float = x_rows.astype(f32)
    centered = x_float - jnp.mean(x_float, axis=-1, keepdims=True)
    inv_std = lax.rsqrt(jnp.mean(centered * centered, axis=-1, keepdims=True) + LN_EPS)
    x_hat = centered * inv_std
    hidden = (x_hat * ln_weight.astype(f32) + ln_bias.astype(f32)).astype(bf16)
    return hidden, x_hat, inv_std


def layer_norm_back(grad_h, x_hat, inv_std, ln_weight):
    scaled = grad_h * ln_weight.astype(f32)
    return inv_std * (scaled - jnp.mean(scaled, axis=-1, keepdims=True)
                      - x_hat * jnp.mean(scaled * x_hat, axis=-1, keepdims=True))


def masked_gate(logits, allowed, choice):
    expert_ids = jnp.arange(logits.shape[-1])
    prob_all = jax.nn.softmax(jnp.where(allowed, logits, -1e30), axis=-1)
    picked = (choice[:, None] == expert_ids[None, :]).astype(f32)
    return jnp.sum(prob_all * picked, axis=-1), prob_all, picked


def solution(mesh):
    n_ep = mesh.shape['ep']
    n_dp = mesh.shape['dp']
    tok_spec = P(('dp', 'ep'), None)
    row_spec = P(('dp', 'ep'))
    exp_spec = P('ep', None, None)
    far = [(i, i ^ 2) for i in range(n_dp)]
    near = [(i, i ^ 1) for i in range(n_dp)]

    def local_step(tok_x, tok_dy, exp_first, exp_second, eligible, slot_first, slot_second,
                   ln_weight, ln_bias, router, w_gate, w_up, w_down):
        n_local, d_model = tok_x.shape
        n_exp = eligible.shape[1]
        slot_cap = 3 * n_local // n_exp
        n_rows = n_exp * slot_cap
        wg_t = w_gate[0].T
        wu_t = w_up[0].T
        wd = w_down[0]

        hidden, x_hat, inv_std = layer_norm(tok_x, ln_weight, ln_bias)
        logits = jnp.dot(hidden, router, preferred_element_type=f32)
        expert_ids = jnp.arange(n_exp)
        allowed = eligible > 0
        gate_one, prob_one, pick_one = masked_gate(logits, allowed, exp_first)
        gate_two, prob_two, pick_two = masked_gate(logits, allowed & (expert_ids[None, :] != exp_first[:, None]), exp_second)
        pos_one = jnp.where(slot_first >= 0, exp_first * slot_cap + slot_first, -1)
        pos_two = jnp.where(slot_second >= 0, exp_second * slot_cap + slot_second, -1)
        meta = jnp.stack([pos_one.astype(f32), pos_two.astype(f32), gate_one, gate_two])
        row_ids = jnp.arange(n_rows)

        def dispatch(h, dy, meta):
            p1 = meta[0].astype(jnp.int32)
            p2 = meta[1].astype(jnp.int32)
            m1 = p1[None, :] == row_ids[:, None]
            m2 = p2[None, :] == row_ids[:, None]
            sel = (m1 | m2).astype(bf16)
            g_row = jnp.sum(jnp.where(m1, meta[2][None, :], 0.0) + jnp.where(m2, meta[3][None, :], 0.0), axis=1)
            h_buf = jnp.dot(sel, h, preferred_element_type=f32).astype(bf16)
            q_buf = (g_row[:, None] * jnp.dot(sel, dy, preferred_element_type=f32)).astype(bf16)
            return h_buf, q_buf

        def swap(buf):
            return lax.all_to_all(buf.reshape(n_ep, slot_cap, d_model), 'ep', 0, 0, tiled=True).reshape(n_rows, d_model)

        def inner(h, q):
            pre_gate = jnp.einsum('rd,fd->rf', h, wg_t, preferred_element_type=f32)
            pre_up = jnp.einsum('rd,fd->rf', h, wu_t, preferred_element_type=f32)
            sig_gate = jax.nn.sigmoid(pre_gate)
            silu_gate = pre_gate * sig_gate
            u = (silu_gate * pre_up).astype(bf16)
            du = jnp.einsum('rd,fd->rf', q, wd, preferred_element_type=f32)
            da = (du * pre_up * sig_gate * (1.0 + pre_gate * (1.0 - sig_gate))).astype(bf16)
            db = (du * silu_gate).astype(bf16)
            return u, da, db

        def dw(u, da, db, h, q):
            def mm(a, b):
                return jnp.einsum('rf,rd->fd', a, b, preferred_element_type=f32)
            return mm(da, h), mm(db, h), mm(u, q)

        dy_f1 = lax.ppermute(tok_dy, 'dp', far)
        h_f1 = lax.ppermute(hidden, 'dp', far)
        m_f1 = lax.ppermute(meta, 'dp', far)
        dy_f2 = lax.ppermute(dy_f1, 'dp', near)
        h_f2 = lax.ppermute(h_f1, 'dp', near)
        m_f2 = lax.ppermute(m_f1, 'dp', near)

        h_buf, q_buf = dispatch(hidden, tok_dy, meta)
        h_own = swap(h_buf)
        q_own = swap(q_buf)
        h_near = lax.ppermute(h_own, 'dp', near)
        q_near = lax.ppermute(q_own, 'dp', near)
        u, da, db = inner(h_own, q_own)
        exp_out = jnp.dot(u, wd, preferred_element_type=f32).astype(bf16)
        grad_hid = (jnp.dot(da, wg_t, preferred_element_type=f32)
                    + jnp.dot(db, wu_t, preferred_element_type=f32)).astype(bf16)
        dwg, dwu, dwd = dw(u, da, db, h_own, q_own)

        h_b1, q_b1 = dispatch(h_f1, dy_f1, m_f1)
        h_b2, q_b2 = dispatch(h_f2, dy_f2, m_f2)
        out_back = swap(exp_out)
        hid_back = swap(grad_hid)
        h_r1, q_r1 = swap(h_b1), swap(q_b1)
        h_r2, q_r2 = swap(h_b2), swap(q_b2)
        for h, q in ((h_r1, q_r1), (h_r2, q_r2), (h_near, q_near)):
            a, b, c = dw(*inner(h, q), h, q)
            dwg, dwu, dwd = dwg + a, dwu + b, dwd + c

        sel_one = (pos_one[:, None] == row_ids[None, :]).astype(bf16)
        sel_two = (pos_two[:, None] == row_ids[None, :]).astype(bf16)
        out_one = jnp.dot(sel_one, out_back, preferred_element_type=f32)
        out_two = jnp.dot(sel_two, out_back, preferred_element_type=f32)
        out_tok = (tok_x.astype(f32) + gate_one[:, None] * out_one + gate_two[:, None] * out_two).astype(bf16)
        dy_float = tok_dy.astype(f32)
        dgate_one = jnp.sum(dy_float * out_one, axis=-1)
        dgate_two = jnp.sum(dy_float * out_two, axis=-1)
        d_logits = ((dgate_one * gate_one)[:, None] * (pick_one - prob_one)
                    + (dgate_two * gate_two)[:, None] * (pick_two - prob_two)).astype(bf16)
        d_router = jnp.einsum('td,te->de', hidden, d_logits, preferred_element_type=f32)
        grad_exp = jnp.dot(sel_one + sel_two, hid_back, preferred_element_type=f32)
        grad_h = jnp.einsum('te,de->td', d_logits, router, preferred_element_type=f32) + grad_exp
        d_ln_weight = jnp.sum(grad_h * x_hat, axis=0)
        d_ln_bias = jnp.sum(grad_h, axis=0)
        dx_tok = (dy_float + layer_norm_back(grad_h, x_hat, inv_std, ln_weight)).astype(bf16)
        d_router = lax.psum(d_router, ('dp', 'ep'))
        d_ln_weight = lax.psum(d_ln_weight, ('dp', 'ep'))
        d_ln_bias = lax.psum(d_ln_bias, ('dp', 'ep'))
        return (out_tok, dx_tok, dwg.T[None], dwu.T[None], dwd[None], d_router, d_ln_weight, d_ln_bias)

    return jax.shard_map(
        local_step, mesh=mesh,
        in_specs=(tok_spec, tok_spec, row_spec, row_spec, tok_spec, row_spec, row_spec,
                  P(), P(), P(), exp_spec, exp_spec, exp_spec),
        out_specs=(tok_spec, tok_spec, exp_spec, exp_spec, exp_spec, P(), P(), P()),
        check_vma=False)
```

```python
import functools

import jax
import jax.numpy as jnp
from jax import lax
from jax.experimental import pallas as pl
from jax.experimental.pallas import tpu as pltpu
from jax.sharding import PartitionSpec as P


LN_EPS = 1e-5
f32 = jnp.float32
bf16 = jnp.bfloat16


def layer_norm(x_rows, ln_weight, ln_bias):
    x_float = x_rows.astype(f32)
    centered = x_float - jnp.mean(x_float, axis=-1, keepdims=True)
    inv_std = lax.rsqrt(jnp.mean(centered * centered, axis=-1, keepdims=True) + LN_EPS)
    x_hat = centered * inv_std
    hidden = (x_hat * ln_weight.astype(f32) + ln_bias.astype(f32)).astype(bf16)
    return hidden, x_hat, inv_std


def layer_norm_back(grad_h, x_hat, inv_std, ln_weight):
    scaled = grad_h * ln_weight.astype(f32)
    return inv_std * (scaled - jnp.mean(scaled, axis=-1, keepdims=True)
                      - x_hat * jnp.mean(scaled * x_hat, axis=-1, keepdims=True))


def masked_gate(logits, allowed, choice):
    expert_ids = jnp.arange(logits.shape[-1])
    prob_all = jax.nn.softmax(jnp.where(allowed, logits, -1e30), axis=-1)
    picked = (choice[:, None] == expert_ids[None, :]).astype(f32)
    return jnp.sum(prob_all * picked, axis=-1), prob_all, picked


VMEM_LIMIT = 63 * 1024 * 1024


def grad_kernel(q_ref, wd_ref, a_ref, b_ref, u_ref, da_ref, db_ref):
    du = lax.dot_general(wd_ref[...], q_ref[...], (((1,), (1,)), ((), ())), preferred_element_type=f32)
    pre_gate = a_ref[...]
    pre_up = b_ref[...]
    sig_gate = jax.nn.sigmoid(pre_gate)
    silu_gate = pre_gate * sig_gate
    u_ref[...] = (silu_gate * pre_up).astype(bf16)
    da_ref[...] = (du * pre_up * sig_gate * (1.0 + pre_gate * (1.0 - sig_gate))).astype(bf16)
    db_ref[...] = (du * silu_gate).astype(bf16)


def inner_grad(q, wd, a_t, b_t):
    n_rows, d_model = q.shape
    width = wd.shape[0]
    w_tile, r_tile = width // 2, n_rows // 3
    tile = pl.BlockSpec((w_tile, r_tile), lambda i, j: (i, j))
    return pl.pallas_call(
        grad_kernel,
        grid=(2, 3),
        in_specs=[pl.BlockSpec((r_tile, d_model), lambda i, j: (j, 0)),
                  pl.BlockSpec((w_tile, d_model), lambda i, j: (i, 0)),
                  tile, tile],
        out_specs=[tile] * 3,
        out_shape=[jax.ShapeDtypeStruct((width, n_rows), bf16)] * 3,
        compiler_params=pltpu.CompilerParams(vmem_limit_bytes=VMEM_LIMIT),
        cost_estimate=pl.CostEstimate(flops=2 * n_rows * d_model * width, bytes_accessed=4 * n_rows * d_model + 14 * width * n_rows,
                                      transcendentals=2 * n_rows * width),
    )(q, wd, a_t, b_t)


def dw_kernel(first, *refs):
    u_ref, da_ref, db_ref, h_ref, q_ref = refs[:5]
    acc = refs[5:-3]
    outs = refs[-3:]
    for k, (left, right) in enumerate(((da_ref, h_ref), (db_ref, h_ref), (u_ref, q_ref))):
        term = jnp.dot(left[...], right[...], preferred_element_type=f32)
        outs[k][...] = term if first else acc[k][...] + term


def add_dw(acc, u_t, da_t, db_t, h, q):
    width, n_rows = u_t.shape
    d_model = h.shape[1]
    first = acc is None
    acc = [] if first else list(acc)
    d_tile = 512
    whole = pl.BlockSpec((width, n_rows), lambda j: (0, 0), pipeline_mode=pl.Buffered(1))
    rows = pl.BlockSpec((n_rows, d_tile), lambda j: (0, j))
    tile = pl.BlockSpec((width, d_tile), lambda j: (0, j))
    return pl.pallas_call(
        functools.partial(dw_kernel, first),
        grid=(d_model // d_tile,),
        in_specs=[whole] * 3 + [rows] * 2 + [tile] * len(acc),
        out_specs=[tile] * 3,
        out_shape=[jax.ShapeDtypeStruct((width, d_model), f32)] * 3,
        input_output_aliases={5 + k: k for k in range(len(acc))},
        compiler_params=pltpu.CompilerParams(vmem_limit_bytes=VMEM_LIMIT),
        cost_estimate=pl.CostEstimate(flops=6 * n_rows * d_model * width, bytes_accessed=4 * n_rows * d_model + 12 * width * d_model * (1 if first else 2),
                                      transcendentals=0),
    )(u_t, da_t, db_t, h, q, *acc)


def after(value, *deps):
    return lax.optimization_barrier((value,) + deps)[0]


def solution(mesh):
    n_ep = mesh.shape['ep']
    n_dp = mesh.shape['dp']
    tok_spec = P(('dp', 'ep'), None)
    row_spec = P(('dp', 'ep'))
    exp_spec = P('ep', None, None)
    outer = [(i, i ^ 2) for i in (0, n_dp - 1)]
    middle = [(i, i ^ 2) for i in (1, n_dp - 2)]
    near = [(i, i ^ 1) for i in range(n_dp)]

    def local_step(tok_x, tok_dy, exp_first, exp_second, eligible, slot_first, slot_second,
                   ln_weight, ln_bias, router, w_gate, w_up, w_down):
        n_local, d_model = tok_x.shape
        n_exp = eligible.shape[1]
        slot_cap = 3 * n_local // n_exp
        n_rows = n_exp * slot_cap
        wg_t = w_gate[0].T
        wu_t = w_up[0].T
        wd = w_down[0]

        hidden, x_hat, inv_std = layer_norm(tok_x, ln_weight, ln_bias)
        logits = jnp.dot(hidden, router, preferred_element_type=f32)
        expert_ids = jnp.arange(n_exp)
        allowed = eligible > 0
        gate_one, prob_one, pick_one = masked_gate(logits, allowed, exp_first)
        gate_two, prob_two, pick_two = masked_gate(logits, allowed & (expert_ids[None, :] != exp_first[:, None]), exp_second)
        pos_one = jnp.where(slot_first >= 0, exp_first * slot_cap + slot_first, -1)
        pos_two = jnp.where(slot_second >= 0, exp_second * slot_cap + slot_second, -1)
        meta = jnp.stack([pos_one.astype(f32), pos_two.astype(f32), gate_one, gate_two])
        row_ids = jnp.arange(n_rows)

        def masks(meta):
            return [meta[k].astype(jnp.int32)[None, :] == row_ids[:, None] for k in range(2)]

        def select_h(h, meta):
            m1, m2 = masks(meta)
            return jnp.dot((m1 | m2).astype(bf16), h, preferred_element_type=f32).astype(bf16)

        def select_q(dy, meta):
            m1, m2 = masks(meta)
            g_row = jnp.sum(jnp.where(m1, meta[2][None, :], 0.0) + jnp.where(m2, meta[3][None, :], 0.0), axis=1)
            return (g_row[:, None] * jnp.dot((m1 | m2).astype(bf16), dy, preferred_element_type=f32)).astype(bf16)

        def swap(buf):
            return lax.all_to_all(buf.reshape(n_ep, slot_cap, d_model), 'ep', 0, 0, tiled=True).reshape(n_rows, d_model)

        def pre(h):
            return (jnp.einsum('fd,rd->fr', wg_t, h, preferred_element_type=f32),
                    jnp.einsum('fd,rd->fr', wu_t, h, preferred_element_type=f32))

        own_meta = jnp.stack([pos_one.astype(f32), pos_two.astype(f32)])
        h_buf = select_h(hidden, own_meta)
        h_own = swap(h_buf)
        dy_a = lax.ppermute(tok_dy, 'dp', outer)
        m_a = lax.ppermute(meta, 'dp', outer)
        h_a = lax.ppermute(after(hidden, meta), 'dp', outer)
        dy_b = lax.ppermute(after(tok_dy, dy_a), 'dp', middle)
        m_b = lax.ppermute(after(meta, m_a), 'dp', middle)
        h_b = lax.ppermute(after(hidden, h_a), 'dp', middle)

        q_buf = select_q(tok_dy, meta)
        q_own = swap(after(q_buf, h_own))
        h_near = lax.ppermute(h_own, 'dp', near)
        a_t, b_t = pre(h_own)
        u_t = (a_t * jax.nn.sigmoid(a_t) * b_t).astype(bf16)
        exp_out = jnp.einsum('fr,fd->rd', u_t, wd, preferred_element_type=f32).astype(bf16)
        out_back = swap(after(exp_out, q_own))
        u_t, da_t, db_t = inner_grad(q_own, wd, a_t, b_t)
        grad_hid = (jnp.einsum('fr,fd->rd', da_t, wg_t, preferred_element_type=f32)
                    + jnp.einsum('fr,fd->rd', db_t, wu_t, preferred_element_type=f32)).astype(bf16)
        acc = add_dw(None, u_t, da_t, db_t, h_own, q_own)

        h_f1, dy_f1, m_f1 = h_a + h_b, dy_a + dy_b, m_a + m_b
        m_f2 = lax.ppermute(m_f1, 'dp', near)
        h_f2 = lax.ppermute(after(h_f1, m_f1), 'dp', near)
        dy_f2 = lax.ppermute(after(dy_f1, h_f1), 'dp', near)
        q_near = lax.ppermute(q_own, 'dp', near)
        h_b1 = select_h(h_f1, m_f1)
        q_b1 = select_q(dy_f1, m_f1)
        h_b2 = select_h(h_f2, m_f2)
        q_b2 = select_q(dy_f2, m_f2)
        h_r1 = swap(after(h_b1, out_back))
        q_r1 = swap(after(q_b1, h_r1))
        h_r2 = swap(after(h_b2, q_r1))
        q_r2 = swap(after(q_b2, h_r2))
        hid_back = swap(after(grad_hid, q_r2))
        for h, q in ((h_r1, q_r1), (h_near, q_near), (h_r2, q_r2)):
            a_t, b_t = pre(h)
            u_t, da_t, db_t = inner_grad(q, wd, a_t, b_t)
            acc = add_dw(acc, u_t, da_t, db_t, h, q)
        dwg, dwu, dwd = acc

        dy_float = tok_dy.astype(f32)
        sel_one = (pos_one[:, None] == row_ids[None, :]).astype(bf16)
        sel_two = (pos_two[:, None] == row_ids[None, :]).astype(bf16)
        out_one = jnp.dot(sel_one, out_back, preferred_element_type=f32)
        out_two = jnp.dot(sel_two, out_back, preferred_element_type=f32)
        out_tok = (tok_x.astype(f32) + gate_one[:, None] * out_one + gate_two[:, None] * out_two).astype(bf16)
        dgate_one = jnp.sum(dy_float * out_one, axis=-1)
        dgate_two = jnp.sum(dy_float * out_two, axis=-1)
        d_logits = ((dgate_one * gate_one)[:, None] * (pick_one - prob_one)
                    + (dgate_two * gate_two)[:, None] * (pick_two - prob_two)).astype(bf16)
        d_router = jnp.einsum('td,te->de', hidden, d_logits, preferred_element_type=f32)
        grad_exp = jnp.dot(sel_one + sel_two, hid_back, preferred_element_type=f32)
        grad_h = jnp.einsum('te,de->td', d_logits, router, preferred_element_type=f32) + grad_exp
        d_ln_weight = jnp.sum(grad_h * x_hat, axis=0)
        d_ln_bias = jnp.sum(grad_h, axis=0)
        dx_tok = (dy_float + layer_norm_back(grad_h, x_hat, inv_std, ln_weight)).astype(bf16)
        d_router = lax.psum(d_router, ('dp', 'ep'))
        d_ln_weight = lax.psum(d_ln_weight, ('dp', 'ep'))
        d_ln_bias = lax.psum(d_ln_bias, ('dp', 'ep'))
        return (out_tok, dx_tok, dwg.T[None], dwu.T[None], dwd[None], d_router, d_ln_weight, d_ln_bias)

    return jax.shard_map(
        local_step, mesh=mesh,
        in_specs=(tok_spec, tok_spec, row_spec, row_spec, tok_spec, row_spec, row_spec,
                  P(), P(), P(), exp_spec, exp_spec, exp_spec),
        out_specs=(tok_spec, tok_spec, exp_spec, exp_spec, exp_spec, P(), P(), P()),
        check_vma=False)
```

```python
import functools

import jax
import jax.numpy as jnp
from jax import lax
from jax.experimental import pallas as pl
from jax.experimental.pallas import tpu as pltpu
from jax.sharding import PartitionSpec as P


LN_EPS = 1e-5
f32 = jnp.float32
bf16 = jnp.bfloat16


def layer_norm(x_rows, ln_weight, ln_bias):
    x_float = x_rows.astype(f32)
    centered = x_float - jnp.mean(x_float, axis=-1, keepdims=True)
    inv_std = lax.rsqrt(jnp.mean(centered * centered, axis=-1, keepdims=True) + LN_EPS)
    x_hat = centered * inv_std
    hidden = (x_hat * ln_weight.astype(f32) + ln_bias.astype(f32)).astype(bf16)
    return hidden, x_hat, inv_std


def layer_norm_back(grad_h, x_hat, inv_std, ln_weight):
    scaled = grad_h * ln_weight.astype(f32)
    return inv_std * (scaled - jnp.mean(scaled, axis=-1, keepdims=True)
                      - x_hat * jnp.mean(scaled * x_hat, axis=-1, keepdims=True))


def masked_gate(logits, allowed, choice):
    expert_ids = jnp.arange(logits.shape[-1])
    prob_all = jax.nn.softmax(jnp.where(allowed, logits, -1e30), axis=-1)
    picked = (choice[:, None] == expert_ids[None, :]).astype(f32)
    return jnp.sum(prob_all * picked, axis=-1), prob_all, picked


VMEM_LIMIT = 63 * 1024 * 1024


def grad_kernel(q_ref, wd_ref, a_ref, b_ref, u_ref, da_ref, db_ref):
    du = lax.dot_general(wd_ref[...], q_ref[...], (((1,), (1,)), ((), ())), preferred_element_type=f32)
    pre_gate = a_ref[...]
    pre_up = b_ref[...]
    sig_gate = jax.nn.sigmoid(pre_gate)
    silu_gate = pre_gate * sig_gate
    u_ref[...] = (silu_gate * pre_up).astype(bf16)
    da_ref[...] = (du * pre_up * sig_gate * (1.0 + pre_gate * (1.0 - sig_gate))).astype(bf16)
    db_ref[...] = (du * silu_gate).astype(bf16)


def inner_grad(q, wd, a_t, b_t):
    n_rows, d_model = q.shape
    width = wd.shape[0]
    w_tile, r_tile = width // 2, n_rows // 3
    tile = pl.BlockSpec((w_tile, r_tile), lambda i, j: (i, j))
    return pl.pallas_call(
        grad_kernel,
        grid=(2, 3),
        in_specs=[pl.BlockSpec((r_tile, d_model), lambda i, j: (j, 0)),
                  pl.BlockSpec((w_tile, d_model), lambda i, j: (i, 0)),
                  tile, tile],
        out_specs=[tile] * 3,
        out_shape=[jax.ShapeDtypeStruct((width, n_rows), bf16)] * 3,
        compiler_params=pltpu.CompilerParams(vmem_limit_bytes=VMEM_LIMIT),
        cost_estimate=pl.CostEstimate(flops=2 * n_rows * d_model * width, bytes_accessed=4 * n_rows * d_model + 14 * width * n_rows,
                                      transcendentals=2 * n_rows * width),
    )(q, wd, a_t, b_t)


def dw_kernel(first, *refs):
    u_ref, da_ref, db_ref, h_ref, q_ref = refs[:5]
    acc = refs[5:-3]
    outs = refs[-3:]
    for k, (left, right) in enumerate(((da_ref, h_ref), (db_ref, h_ref), (u_ref, q_ref))):
        term = jnp.dot(left[...], right[...], preferred_element_type=f32)
        outs[k][...] = term if first else acc[k][...] + term


def add_dw(acc, u_t, da_t, db_t, h, q):
    width, n_rows = u_t.shape
    d_model = h.shape[1]
    first = acc is None
    acc = [] if first else list(acc)
    d_tile = 512
    whole = pl.BlockSpec((width, n_rows), lambda j: (0, 0), pipeline_mode=pl.Buffered(1))
    rows = pl.BlockSpec((n_rows, d_tile), lambda j: (0, j))
    tile = pl.BlockSpec((width, d_tile), lambda j: (0, j))
    return pl.pallas_call(
        functools.partial(dw_kernel, first),
        grid=(d_model // d_tile,),
        in_specs=[whole] * 3 + [rows] * 2 + [tile] * len(acc),
        out_specs=[tile] * 3,
        out_shape=[jax.ShapeDtypeStruct((width, d_model), f32)] * 3,
        input_output_aliases={5 + k: k for k in range(len(acc))},
        compiler_params=pltpu.CompilerParams(vmem_limit_bytes=VMEM_LIMIT),
        cost_estimate=pl.CostEstimate(flops=6 * n_rows * d_model * width, bytes_accessed=4 * n_rows * d_model + 12 * width * d_model * (1 if first else 2),
                                      transcendentals=0),
    )(u_t, da_t, db_t, h, q, *acc)


def sum_kernel(n_dp, n_ep, x_ref, out_ref, parts, total, send_one, recv_one, send_two, recv_two):
    n_dev = n_dp * n_ep
    me = lax.axis_index('dp') * n_ep + lax.axis_index('ep')

    def peer(step):
        index = lax.rem(me + step, n_dev)
        return index, (lax.div(index, n_ep), lax.rem(index, n_ep))

    scatter = []
    for step in range(1, n_dev):
        index, device = peer(step)
        scatter.append(pltpu.make_async_remote_copy(
            src_ref=x_ref.at[index], dst_ref=parts.at[step], send_sem=send_one.at[step], recv_sem=recv_one.at[step],
            device_id=device, device_id_type=pl.DeviceIdType.MESH))
        scatter[-1].start()
    acc = x_ref[me]
    for step in range(1, n_dev):
        scatter[step - 1].wait_recv()
        acc += parts[step]
    total[...] = acc
    out_ref[me] = acc
    for copy in scatter:
        copy.wait_send()
    gather = []
    for step in range(1, n_dev):
        index, device = peer(step)
        gather.append(pltpu.make_async_remote_copy(
            src_ref=total, dst_ref=out_ref.at[me], send_sem=send_two.at[step], recv_sem=recv_two.at[step],
            device_id=device, device_id_type=pl.DeviceIdType.MESH))
        gather[-1].start()
    for copy in gather:
        copy.wait_recv()
    for copy in gather:
        copy.wait_send()


def sum_all(x, n_dp, n_ep):
    n_dev = n_dp * n_ep
    vmem = pl.BlockSpec(memory_space=pltpu.VMEM)
    dma = pltpu.SemaphoreType.DMA((n_dev,))
    return pl.pallas_call(
        functools.partial(sum_kernel, n_dp, n_ep),
        out_shape=jax.ShapeDtypeStruct(x.shape, f32),
        in_specs=[vmem], out_specs=vmem,
        scratch_shapes=[pltpu.VMEM(x.shape, f32), pltpu.VMEM(x.shape[1:], f32), dma, dma, dma, dma],
        compiler_params=pltpu.CompilerParams(has_side_effects=True),
    )(x)


def after(value, *deps):
    return lax.optimization_barrier((value,) + deps)[0]


def solution(mesh):
    n_ep = mesh.shape['ep']
    n_dp = mesh.shape['dp']
    tok_spec = P(('dp', 'ep'), None)
    row_spec = P(('dp', 'ep'))
    exp_spec = P('ep', None, None)
    outer = [(i, i ^ 2) for i in (0, n_dp - 1)]
    middle = [(i, i ^ 2) for i in (1, n_dp - 2)]
    near = [(i, i ^ 1) for i in range(n_dp)]

    def local_step(tok_x, tok_dy, exp_first, exp_second, eligible, slot_first, slot_second,
                   ln_weight, ln_bias, router, w_gate, w_up, w_down):
        n_local, d_model = tok_x.shape
        n_exp = eligible.shape[1]
        slot_cap = 3 * n_local // n_exp
        n_rows = n_exp * slot_cap
        wg_t = w_gate[0].T
        wu_t = w_up[0].T
        wd = w_down[0]

        hidden, x_hat, inv_std = layer_norm(tok_x, ln_weight, ln_bias)
        logits = jnp.dot(hidden, router, preferred_element_type=f32)
        expert_ids = jnp.arange(n_exp)
        allowed = eligible > 0
        gate_one, prob_one, pick_one = masked_gate(logits, allowed, exp_first)
        gate_two, prob_two, pick_two = masked_gate(logits, allowed & (expert_ids[None, :] != exp_first[:, None]), exp_second)
        pos_one = jnp.where(slot_first >= 0, exp_first * slot_cap + slot_first, -1)
        pos_two = jnp.where(slot_second >= 0, exp_second * slot_cap + slot_second, -1)
        meta = jnp.stack([pos_one.astype(f32), pos_two.astype(f32), gate_one, gate_two])
        row_ids = jnp.arange(n_rows)

        def masks(meta):
            return [meta[k].astype(jnp.int32)[None, :] == row_ids[:, None] for k in range(2)]

        def select_h(h, meta):
            m1, m2 = masks(meta)
            return jnp.dot((m1 | m2).astype(bf16), h, preferred_element_type=f32).astype(bf16)

        def select_q(dy, meta):
            m1, m2 = masks(meta)
            g_row = jnp.sum(jnp.where(m1, meta[2][None, :], 0.0) + jnp.where(m2, meta[3][None, :], 0.0), axis=1)
            return (g_row[:, None] * jnp.dot((m1 | m2).astype(bf16), dy, preferred_element_type=f32)).astype(bf16)

        def swap(buf):
            return lax.all_to_all(buf.reshape(n_ep, slot_cap, d_model), 'ep', 0, 0, tiled=True).reshape(n_rows, d_model)

        def pre(h):
            return (jnp.einsum('fd,rd->fr', wg_t, h, preferred_element_type=f32),
                    jnp.einsum('fd,rd->fr', wu_t, h, preferred_element_type=f32))

        own_meta = jnp.stack([pos_one.astype(f32), pos_two.astype(f32)])
        h_buf = select_h(hidden, own_meta)
        h_own = swap(h_buf)
        m_f1 = lax.ppermute(meta, 'dp', outer + middle)
        h_f1 = lax.ppermute(hidden, 'dp', outer + middle)
        dy_a = lax.ppermute(tok_dy, 'dp', outer)
        dy_b = lax.ppermute(after(tok_dy, dy_a), 'dp', middle)
        q_buf = select_q(tok_dy, meta)
        q_own = swap(after(q_buf, h_own))
        a_t, b_t = pre(h_own)
        u_t = (a_t * jax.nn.sigmoid(a_t) * b_t).astype(bf16)
        exp_out = jnp.einsum('fr,fd->rd', u_t, wd, preferred_element_type=f32).astype(bf16)
        u_t, da_t, db_t = inner_grad(q_own, wd, a_t, b_t)
        grad_hid = (jnp.einsum('fr,fd->rd', da_t, wg_t, preferred_element_type=f32)
                    + jnp.einsum('fr,fd->rd', db_t, wu_t, preferred_element_type=f32)).astype(bf16)
        acc = add_dw(None, u_t, da_t, db_t, h_own, q_own)

        dy_f1 = dy_a + dy_b
        m_f2 = lax.ppermute(m_f1, 'dp', near)
        h_f2 = lax.ppermute(h_f1, 'dp', near)
        dy_f2 = lax.ppermute(dy_f1, 'dp', near)
        h_near = lax.ppermute(h_own, 'dp', near)
        q_near = lax.ppermute(q_own, 'dp', near)
        h_b1 = select_h(h_f1, m_f1)
        q_b1 = select_q(dy_f1, m_f1)
        h_b2 = select_h(h_f2, m_f2)
        q_b2 = select_q(dy_f2, m_f2)
        h_r1 = swap(after(h_b1, q_own))
        q_r1 = swap(after(q_b1, h_r1))
        h_r2 = swap(after(h_b2, q_r1))
        q_r2 = swap(after(q_b2, h_r2))
        out_back = swap(after(exp_out, q_r2))
        hid_back = swap(after(grad_hid, out_back))
        for h, q in ((h_r1, q_r1), (h_r2, q_r2), (h_near, q_near)):
            a_t, b_t = pre(h)
            u_t, da_t, db_t = inner_grad(q, wd, a_t, b_t)
            acc = add_dw(acc, u_t, da_t, db_t, h, q)
        dwg, dwu, dwd = acc

        dy_float = tok_dy.astype(f32)
        sel_one = (pos_one[:, None] == row_ids[None, :]).astype(bf16)
        sel_two = (pos_two[:, None] == row_ids[None, :]).astype(bf16)
        out_one = jnp.dot(sel_one, out_back, preferred_element_type=f32)
        out_two = jnp.dot(sel_two, out_back, preferred_element_type=f32)
        out_tok = (tok_x.astype(f32) + gate_one[:, None] * out_one + gate_two[:, None] * out_two).astype(bf16)
        dgate_one = jnp.sum(dy_float * out_one, axis=-1)
        dgate_two = jnp.sum(dy_float * out_two, axis=-1)
        d_logits = ((dgate_one * gate_one)[:, None] * (pick_one - prob_one)
                    + (dgate_two * gate_two)[:, None] * (pick_two - prob_two)).astype(bf16)
        d_router = jnp.einsum('td,te->ed', hidden, d_logits, preferred_element_type=f32)
        grad_exp = jnp.dot(sel_one + sel_two, hid_back, preferred_element_type=f32)
        grad_h = jnp.einsum('te,de->td', d_logits, router, preferred_element_type=f32) + grad_exp
        d_ln_weight = jnp.sum(grad_h * x_hat, axis=0)
        d_ln_bias = jnp.sum(grad_h, axis=0)
        dx_tok = (dy_float + layer_norm_back(grad_h, x_hat, inv_std, ln_weight)).astype(bf16)
        n_dev = n_dp * n_ep
        parts = jnp.concatenate([d_router, d_ln_weight[None], d_ln_bias[None], jnp.zeros((6, d_model), f32)])
        total = sum_all(parts.reshape(16, n_dev, d_model // n_dev).transpose(1, 0, 2), n_dp, n_ep)
        total = total.transpose(1, 0, 2).reshape(16, d_model)
        d_router, d_ln_weight, d_ln_bias = total[:n_exp].T, total[n_exp], total[n_exp + 1]
        return (out_tok, dx_tok, dwg.T[None], dwu.T[None], dwd[None], d_router, d_ln_weight, d_ln_bias)

    return jax.shard_map(
        local_step, mesh=mesh,
        in_specs=(tok_spec, tok_spec, row_spec, row_spec, tok_spec, row_spec, row_spec,
                  P(), P(), P(), exp_spec, exp_spec, exp_spec),
        out_specs=(tok_spec, tok_spec, exp_spec, exp_spec, exp_spec, P(), P(), P()),
        check_vma=False)
```

```python
import functools

import jax
import jax.numpy as jnp
from jax import lax
from jax.experimental import pallas as pl
from jax.experimental.pallas import tpu as pltpu
from jax.sharding import PartitionSpec as P


LN_EPS = 1e-5
f32 = jnp.float32
bf16 = jnp.bfloat16


def layer_norm(x_rows, ln_weight, ln_bias):
    x_float = x_rows.astype(f32)
    centered = x_float - jnp.mean(x_float, axis=-1, keepdims=True)
    inv_std = lax.rsqrt(jnp.mean(centered * centered, axis=-1, keepdims=True) + LN_EPS)
    x_hat = centered * inv_std
    hidden = (x_hat * ln_weight.astype(f32) + ln_bias.astype(f32)).astype(bf16)
    return hidden, x_hat, inv_std


def layer_norm_back(grad_h, x_hat, inv_std, ln_weight):
    scaled = grad_h * ln_weight.astype(f32)
    return inv_std * (scaled - jnp.mean(scaled, axis=-1, keepdims=True)
                      - x_hat * jnp.mean(scaled * x_hat, axis=-1, keepdims=True))


def masked_gate(logits, allowed, choice):
    expert_ids = jnp.arange(logits.shape[-1])
    prob_all = jax.nn.softmax(jnp.where(allowed, logits, -1e30), axis=-1)
    picked = (choice[:, None] == expert_ids[None, :]).astype(f32)
    return jnp.sum(prob_all * picked, axis=-1), prob_all, picked


VMEM_LIMIT = 63 * 1024 * 1024


def grad_kernel(q_ref, wd_ref, a_ref, b_ref, u_ref, da_ref, db_ref):
    du = lax.dot_general(wd_ref[...], q_ref[...], (((1,), (1,)), ((), ())), preferred_element_type=f32)
    pre_gate = a_ref[...]
    pre_up = b_ref[...]
    sig_gate = jax.nn.sigmoid(pre_gate)
    silu_gate = pre_gate * sig_gate
    u_ref[...] = (silu_gate * pre_up).astype(bf16)
    da_ref[...] = (du * pre_up * sig_gate * (1.0 + pre_gate * (1.0 - sig_gate))).astype(bf16)
    db_ref[...] = (du * silu_gate).astype(bf16)


def inner_grad(q, wd, a_t, b_t):
    n_rows, d_model = q.shape
    width = wd.shape[0]
    w_tile, r_tile = width // 2, n_rows // 3
    tile = pl.BlockSpec((w_tile, r_tile), lambda i, j: (i, j))
    return pl.pallas_call(
        grad_kernel,
        grid=(2, 3),
        in_specs=[pl.BlockSpec((r_tile, d_model), lambda i, j: (j, 0)),
                  pl.BlockSpec((w_tile, d_model), lambda i, j: (i, 0)),
                  tile, tile],
        out_specs=[tile] * 3,
        out_shape=[jax.ShapeDtypeStruct((width, n_rows), bf16)] * 3,
        compiler_params=pltpu.CompilerParams(vmem_limit_bytes=VMEM_LIMIT),
        cost_estimate=pl.CostEstimate(flops=2 * n_rows * d_model * width, bytes_accessed=4 * n_rows * d_model + 14 * width * n_rows,
                                      transcendentals=2 * n_rows * width),
    )(q, wd, a_t, b_t)


def dw_kernel(first, *refs):
    u_ref, da_ref, db_ref, h_ref, q_ref = refs[:5]
    acc = refs[5:-3]
    outs = refs[-3:]
    for k, (left, right) in enumerate(((da_ref, h_ref), (db_ref, h_ref), (u_ref, q_ref))):
        term = jnp.dot(left[...], right[...], preferred_element_type=f32)
        outs[k][...] = term if first else acc[k][...] + term


def add_dw(acc, u_t, da_t, db_t, h, q):
    width, n_rows = u_t.shape
    d_model = h.shape[1]
    first = acc is None
    acc = [] if first else list(acc)
    d_tile = 512
    whole = pl.BlockSpec((width, n_rows), lambda j: (0, 0), pipeline_mode=pl.Buffered(1))
    rows = pl.BlockSpec((n_rows, d_tile), lambda j: (0, j))
    tile = pl.BlockSpec((width, d_tile), lambda j: (0, j))
    return pl.pallas_call(
        functools.partial(dw_kernel, first),
        grid=(d_model // d_tile,),
        in_specs=[whole] * 3 + [rows] * 2 + [tile] * len(acc),
        out_specs=[tile] * 3,
        out_shape=[jax.ShapeDtypeStruct((width, d_model), f32)] * 3,
        input_output_aliases={5 + k: k for k in range(len(acc))},
        compiler_params=pltpu.CompilerParams(vmem_limit_bytes=VMEM_LIMIT),
        cost_estimate=pl.CostEstimate(flops=6 * n_rows * d_model * width, bytes_accessed=4 * n_rows * d_model + 12 * width * d_model * (1 if first else 2),
                                      transcendentals=0),
    )(u_t, da_t, db_t, h, q, *acc)


def sum_kernel(n_dp, n_ep, x_ref, out_ref, parts, total, send_one, recv_one, send_two, recv_two):
    n_dev = n_dp * n_ep
    me = lax.axis_index('dp') * n_ep + lax.axis_index('ep')

    def peer(step):
        index = lax.rem(me + step, n_dev)
        return index, (lax.div(index, n_ep), lax.rem(index, n_ep))

    scatter = []
    for step in range(1, n_dev):
        index, device = peer(step)
        scatter.append(pltpu.make_async_remote_copy(
            src_ref=x_ref.at[index], dst_ref=parts.at[step], send_sem=send_one.at[step], recv_sem=recv_one.at[step],
            device_id=device, device_id_type=pl.DeviceIdType.MESH))
        scatter[-1].start()
    acc = x_ref[me]
    for step in range(1, n_dev):
        scatter[step - 1].wait_recv()
        acc += parts[step]
    total[...] = acc
    out_ref[me] = acc
    for copy in scatter:
        copy.wait_send()
    gather = []
    for step in range(1, n_dev):
        index, device = peer(step)
        gather.append(pltpu.make_async_remote_copy(
            src_ref=total, dst_ref=out_ref.at[me], send_sem=send_two.at[step], recv_sem=recv_two.at[step],
            device_id=device, device_id_type=pl.DeviceIdType.MESH))
        gather[-1].start()
    for copy in gather:
        copy.wait_recv()
    for copy in gather:
        copy.wait_send()


def sum_all(x, n_dp, n_ep):
    n_dev = n_dp * n_ep
    vmem = pl.BlockSpec(memory_space=pltpu.VMEM)
    dma = pltpu.SemaphoreType.DMA((n_dev,))
    return pl.pallas_call(
        functools.partial(sum_kernel, n_dp, n_ep),
        out_shape=jax.ShapeDtypeStruct(x.shape, f32),
        in_specs=[vmem], out_specs=vmem,
        scratch_shapes=[pltpu.VMEM(x.shape, f32), pltpu.VMEM(x.shape[1:], f32), dma, dma, dma, dma],
        compiler_params=pltpu.CompilerParams(has_side_effects=True),
    )(x)


def after(value, *deps):
    return lax.optimization_barrier((value,) + deps)[0]


def solution(mesh):
    n_ep = mesh.shape['ep']
    n_dp = mesh.shape['dp']
    tok_spec = P(('dp', 'ep'), None)
    row_spec = P(('dp', 'ep'))
    exp_spec = P('ep', None, None)
    outer = [(i, i ^ 2) for i in (0, n_dp - 1)]
    middle = [(i, i ^ 2) for i in (1, n_dp - 2)]
    near = [(i, i ^ 1) for i in range(n_dp)]

    def local_step(tok_x, tok_dy, exp_first, exp_second, eligible, slot_first, slot_second,
                   ln_weight, ln_bias, router, w_gate, w_up, w_down):
        n_local, d_model = tok_x.shape
        n_exp = eligible.shape[1]
        slot_cap = 3 * n_local // n_exp
        n_rows = n_exp * slot_cap
        wg_t = w_gate[0].T
        wu_t = w_up[0].T
        wd = w_down[0]

        hidden, x_hat, inv_std = layer_norm(tok_x, ln_weight, ln_bias)
        logits = jnp.dot(hidden, router, preferred_element_type=f32)
        expert_ids = jnp.arange(n_exp)
        allowed = eligible > 0
        gate_one, prob_one, pick_one = masked_gate(logits, allowed, exp_first)
        gate_two, prob_two, pick_two = masked_gate(logits, allowed & (expert_ids[None, :] != exp_first[:, None]), exp_second)
        pos_one = jnp.where(slot_first >= 0, exp_first * slot_cap + slot_first, -1)
        pos_two = jnp.where(slot_second >= 0, exp_second * slot_cap + slot_second, -1)
        meta = jnp.stack([pos_one.astype(f32), pos_two.astype(f32), gate_one, gate_two])
        row_ids = jnp.arange(n_rows)

        def masks(meta):
            return [meta[k].astype(jnp.int32)[None, :] == row_ids[:, None] for k in range(2)]

        def select_h(h, meta):
            m1, m2 = masks(meta)
            return jnp.dot((m1 | m2).astype(bf16), h, preferred_element_type=f32).astype(bf16)

        def select_q(dy, meta):
            m1, m2 = masks(meta)
            g_row = jnp.sum(jnp.where(m1, meta[2][None, :], 0.0) + jnp.where(m2, meta[3][None, :], 0.0), axis=1)
            return (g_row[:, None] * jnp.dot((m1 | m2).astype(bf16), dy, preferred_element_type=f32)).astype(bf16)

        def swap(buf):
            return lax.all_to_all(buf.reshape(n_ep, slot_cap, d_model), 'ep', 0, 0, tiled=True).reshape(n_rows, d_model)

        def pre(h):
            return (jnp.einsum('fd,rd->fr', wg_t, h, preferred_element_type=f32),
                    jnp.einsum('fd,rd->fr', wu_t, h, preferred_element_type=f32))

        own_meta = jnp.stack([pos_one.astype(f32), pos_two.astype(f32)])
        h_buf = select_h(hidden, own_meta)
        h_own = swap(h_buf)
        m_f1 = lax.ppermute(meta, 'dp', outer + middle)
        h_f1 = lax.ppermute(hidden, 'dp', outer + middle)
        dy_f1 = lax.ppermute(after(tok_dy, h_f1), 'dp', outer + middle)
        q_buf = select_q(tok_dy, meta)
        q_own = swap(q_buf)
        a_t, b_t = pre(h_own)
        u_t = (a_t * jax.nn.sigmoid(a_t) * b_t).astype(bf16)
        exp_out = jnp.einsum('fr,fd->rd', u_t, wd, preferred_element_type=f32).astype(bf16)
        u_t, da_t, db_t = inner_grad(q_own, wd, a_t, b_t)
        grad_hid = (jnp.einsum('fr,fd->rd', da_t, wg_t, preferred_element_type=f32)
                    + jnp.einsum('fr,fd->rd', db_t, wu_t, preferred_element_type=f32)).astype(bf16)
        acc = add_dw(None, u_t, da_t, db_t, h_own, q_own)

        m_f2 = lax.ppermute(m_f1, 'dp', near)
        h_f2 = lax.ppermute(h_f1, 'dp', near)
        dy_f2 = lax.ppermute(dy_f1, 'dp', near)
        h_near = lax.ppermute(h_own, 'dp', near)
        q_near = lax.ppermute(q_own, 'dp', near)
        h_b1 = select_h(h_f1, m_f1)
        q_b1 = select_q(dy_f1, m_f1)
        h_b2 = select_h(h_f2, m_f2)
        q_b2 = select_q(dy_f2, m_f2)
        h_r1 = swap(h_b1)
        q_r1 = swap(q_b1)
        h_r2 = swap(h_b2)
        q_r2 = swap(q_b2)
        out_back = swap(exp_out)
        hid_back = swap(grad_hid)
        for h, q in ((h_r1, q_r1), (h_r2, q_r2), (h_near, q_near)):
            a_t, b_t = pre(h)
            u_t, da_t, db_t = inner_grad(q, wd, a_t, b_t)
            acc = add_dw(acc, u_t, da_t, db_t, h, q)
        dwg, dwu, dwd = acc

        dy_float = tok_dy.astype(f32)
        sel_one = (pos_one[:, None] == row_ids[None, :]).astype(bf16)
        sel_two = (pos_two[:, None] == row_ids[None, :]).astype(bf16)
        out_one = jnp.dot(sel_one, out_back, preferred_element_type=f32)
        out_two = jnp.dot(sel_two, out_back, preferred_element_type=f32)
        out_tok = (tok_x.astype(f32) + gate_one[:, None] * out_one + gate_two[:, None] * out_two).astype(bf16)
        dgate_one = jnp.sum(dy_float * out_one, axis=-1)
        dgate_two = jnp.sum(dy_float * out_two, axis=-1)
        d_logits = ((dgate_one * gate_one)[:, None] * (pick_one - prob_one)
                    + (dgate_two * gate_two)[:, None] * (pick_two - prob_two)).astype(bf16)
        d_router = jnp.einsum('td,te->ed', hidden, d_logits, preferred_element_type=f32)
        grad_exp = jnp.dot(sel_one + sel_two, hid_back, preferred_element_type=f32)
        grad_h = jnp.einsum('te,de->td', d_logits, router, preferred_element_type=f32) + grad_exp
        d_ln_weight = jnp.sum(grad_h * x_hat, axis=0)
        d_ln_bias = jnp.sum(grad_h, axis=0)
        dx_tok = (dy_float + layer_norm_back(grad_h, x_hat, inv_std, ln_weight)).astype(bf16)
        n_dev = n_dp * n_ep

        def all_sum(rows):
            parts = rows.reshape(rows.shape[0], n_dev, d_model // n_dev).transpose(1, 0, 2)
            return sum_all(parts, n_dp, n_ep).transpose(1, 0, 2).reshape(rows.shape)

        d_router = all_sum(d_router).T
        d_ln_weight, d_ln_bias = all_sum(jnp.stack([d_ln_weight, d_ln_bias]))
        return (out_tok, dx_tok, dwg.T[None], dwu.T[None], dwd[None], d_router, d_ln_weight, d_ln_bias)

    return jax.shard_map(
        local_step, mesh=mesh,
        in_specs=(tok_spec, tok_spec, row_spec, row_spec, tok_spec, row_spec, row_spec,
                  P(), P(), P(), exp_spec, exp_spec, exp_spec),
        out_specs=(tok_spec, tok_spec, exp_spec, exp_spec, exp_spec, P(), P(), P()),
        check_vma=False)
```

```python
import functools

import jax
import jax.numpy as jnp
from jax import lax
from jax.experimental import pallas as pl
from jax.experimental.pallas import tpu as pltpu
from jax.sharding import PartitionSpec as P


LN_EPS = 1e-5
f32 = jnp.float32
bf16 = jnp.bfloat16


def layer_norm(x_rows, ln_weight, ln_bias):
    x_float = x_rows.astype(f32)
    centered = x_float - jnp.mean(x_float, axis=-1, keepdims=True)
    inv_std = lax.rsqrt(jnp.mean(centered * centered, axis=-1, keepdims=True) + LN_EPS)
    x_hat = centered * inv_std
    hidden = (x_hat * ln_weight.astype(f32) + ln_bias.astype(f32)).astype(bf16)
    return hidden, x_hat, inv_std


def layer_norm_back(grad_h, x_hat, inv_std, ln_weight):
    scaled = grad_h * ln_weight.astype(f32)
    return inv_std * (scaled - jnp.mean(scaled, axis=-1, keepdims=True)
                      - x_hat * jnp.mean(scaled * x_hat, axis=-1, keepdims=True))


def masked_gate(logits, allowed, choice):
    expert_ids = jnp.arange(logits.shape[-1])
    prob_all = jax.nn.softmax(jnp.where(allowed, logits, -1e30), axis=-1)
    picked = (choice[:, None] == expert_ids[None, :]).astype(f32)
    return jnp.sum(prob_all * picked, axis=-1), prob_all, picked


VMEM_LIMIT = 63 * 1024 * 1024


def grad_kernel(q_ref, wd_ref, a_ref, b_ref, u_ref, da_ref, db_ref):
    du = lax.dot_general(wd_ref[...], q_ref[...], (((1,), (1,)), ((), ())), preferred_element_type=f32)
    pre_gate = a_ref[...]
    pre_up = b_ref[...]
    sig_gate = jax.nn.sigmoid(pre_gate)
    silu_gate = pre_gate * sig_gate
    u_ref[...] = (silu_gate * pre_up).astype(bf16)
    da_ref[...] = (du * pre_up * sig_gate * (1.0 + pre_gate * (1.0 - sig_gate))).astype(bf16)
    db_ref[...] = (du * silu_gate).astype(bf16)


def inner_grad(q, wd, a_t, b_t):
    n_rows, d_model = q.shape
    width = wd.shape[0]
    r_tile = n_rows // 6
    tile = pl.BlockSpec((width, r_tile), lambda j: (0, j))
    return pl.pallas_call(
        grad_kernel,
        grid=(n_rows // r_tile,),
        in_specs=[pl.BlockSpec((r_tile, d_model), lambda j: (j, 0)),
                  pl.BlockSpec((width, d_model), lambda j: (0, 0), pipeline_mode=pl.Buffered(1)),
                  tile, tile],
        out_specs=[tile] * 3,
        out_shape=[jax.ShapeDtypeStruct((width, n_rows), bf16)] * 3,
        compiler_params=pltpu.CompilerParams(vmem_limit_bytes=VMEM_LIMIT),
        cost_estimate=pl.CostEstimate(flops=2 * n_rows * d_model * width, bytes_accessed=4 * n_rows * d_model + 14 * width * n_rows,
                                      transcendentals=2 * n_rows * width),
    )(q, wd, a_t, b_t)


def dw_kernel(first, *refs):
    u_ref, da_ref, db_ref, h_ref, q_ref = refs[:5]
    acc = refs[5:-3]
    outs = refs[-3:]
    for k, (left, right) in enumerate(((da_ref, h_ref), (db_ref, h_ref), (u_ref, q_ref))):
        term = jnp.dot(left[...], right[...], preferred_element_type=f32)
        outs[k][...] = term if first else acc[k][...] + term


def add_dw(acc, u_t, da_t, db_t, h, q):
    width, n_rows = u_t.shape
    d_model = h.shape[1]
    first = acc is None
    acc = [] if first else list(acc)
    d_tile = 512
    whole = pl.BlockSpec((width, n_rows), lambda j: (0, 0), pipeline_mode=pl.Buffered(1))
    rows = pl.BlockSpec((n_rows, d_tile), lambda j: (0, j))
    tile = pl.BlockSpec((width, d_tile), lambda j: (0, j))
    return pl.pallas_call(
        functools.partial(dw_kernel, first),
        grid=(d_model // d_tile,),
        in_specs=[whole] * 3 + [rows] * 2 + [tile] * len(acc),
        out_specs=[tile] * 3,
        out_shape=[jax.ShapeDtypeStruct((width, d_model), f32)] * 3,
        input_output_aliases={5 + k: k for k in range(len(acc))},
        compiler_params=pltpu.CompilerParams(vmem_limit_bytes=VMEM_LIMIT),
        cost_estimate=pl.CostEstimate(flops=6 * n_rows * d_model * width, bytes_accessed=4 * n_rows * d_model + 12 * width * d_model * (1 if first else 2),
                                      transcendentals=0),
    )(u_t, da_t, db_t, h, q, *acc)


def sum_kernel(n_dp, n_ep, x_ref, out_ref, parts, total, send_one, recv_one, send_two, recv_two):
    n_dev = n_dp * n_ep
    me = lax.axis_index('dp') * n_ep + lax.axis_index('ep')

    def peer(step):
        index = lax.rem(me + step, n_dev)
        return index, (lax.div(index, n_ep), lax.rem(index, n_ep))

    scatter = []
    for step in range(1, n_dev):
        index, device = peer(step)
        scatter.append(pltpu.make_async_remote_copy(
            src_ref=x_ref.at[index], dst_ref=parts.at[step], send_sem=send_one.at[step], recv_sem=recv_one.at[step],
            device_id=device, device_id_type=pl.DeviceIdType.MESH))
        scatter[-1].start()
    acc = x_ref[me]
    for step in range(1, n_dev):
        scatter[step - 1].wait_recv()
        acc += parts[step]
    total[...] = acc
    out_ref[me] = acc
    for copy in scatter:
        copy.wait_send()
    gather = []
    for step in range(1, n_dev):
        index, device = peer(step)
        gather.append(pltpu.make_async_remote_copy(
            src_ref=total, dst_ref=out_ref.at[me], send_sem=send_two.at[step], recv_sem=recv_two.at[step],
            device_id=device, device_id_type=pl.DeviceIdType.MESH))
        gather[-1].start()
    for copy in gather:
        copy.wait_recv()
    for copy in gather:
        copy.wait_send()


def sum_all(x, n_dp, n_ep):
    n_dev = n_dp * n_ep
    vmem = pl.BlockSpec(memory_space=pltpu.VMEM)
    dma = pltpu.SemaphoreType.DMA((n_dev,))
    return pl.pallas_call(
        functools.partial(sum_kernel, n_dp, n_ep),
        out_shape=jax.ShapeDtypeStruct(x.shape, f32),
        in_specs=[vmem], out_specs=vmem,
        scratch_shapes=[pltpu.VMEM(x.shape, f32), pltpu.VMEM(x.shape[1:], f32), dma, dma, dma, dma],
        compiler_params=pltpu.CompilerParams(has_side_effects=True),
    )(x)


def after(value, *deps):
    return lax.optimization_barrier((value,) + deps)[0]


def solution(mesh):
    n_ep = mesh.shape['ep']
    n_dp = mesh.shape['dp']
    tok_spec = P(('dp', 'ep'), None)
    row_spec = P(('dp', 'ep'))
    exp_spec = P('ep', None, None)
    outer = [(i, i ^ 2) for i in (0, n_dp - 1)]
    middle = [(i, i ^ 2) for i in (1, n_dp - 2)]
    near = [(i, i ^ 1) for i in range(n_dp)]

    def local_step(tok_x, tok_dy, exp_first, exp_second, eligible, slot_first, slot_second,
                   ln_weight, ln_bias, router, w_gate, w_up, w_down):
        n_local, d_model = tok_x.shape
        n_exp = eligible.shape[1]
        slot_cap = 3 * n_local // n_exp
        n_rows = n_exp * slot_cap
        wg_t = w_gate[0].T
        wu_t = w_up[0].T
        wd = w_down[0]

        hidden, x_hat, inv_std = layer_norm(tok_x, ln_weight, ln_bias)
        logits = jnp.dot(hidden, router, preferred_element_type=f32)
        expert_ids = jnp.arange(n_exp)
        allowed = eligible > 0
        gate_one, prob_one, pick_one = masked_gate(logits, allowed, exp_first)
        gate_two, prob_two, pick_two = masked_gate(logits, allowed & (expert_ids[None, :] != exp_first[:, None]), exp_second)
        pos_one = jnp.where(slot_first >= 0, exp_first * slot_cap + slot_first, -1)
        pos_two = jnp.where(slot_second >= 0, exp_second * slot_cap + slot_second, -1)
        meta = jnp.stack([pos_one.astype(f32), pos_two.astype(f32), gate_one, gate_two])
        row_ids = jnp.arange(n_rows)

        def masks(meta):
            return [meta[k].astype(jnp.int32)[None, :] == row_ids[:, None] for k in range(2)]

        def select_h(h, meta):
            m1, m2 = masks(meta)
            return jnp.dot((m1 | m2).astype(bf16), h, preferred_element_type=f32).astype(bf16)

        def select_q(dy, meta):
            m1, m2 = masks(meta)
            g_row = jnp.sum(jnp.where(m1, meta[2][None, :], 0.0) + jnp.where(m2, meta[3][None, :], 0.0), axis=1)
            return (g_row[:, None] * jnp.dot((m1 | m2).astype(bf16), dy, preferred_element_type=f32)).astype(bf16)

        def swap(buf):
            return lax.all_to_all(buf.reshape(n_ep, slot_cap, d_model), 'ep', 0, 0, tiled=True).reshape(n_rows, d_model)

        def pre(h):
            return (jnp.einsum('fd,rd->fr', wg_t, h, preferred_element_type=f32),
                    jnp.einsum('fd,rd->fr', wu_t, h, preferred_element_type=f32))

        own_meta = jnp.stack([pos_one.astype(f32), pos_two.astype(f32)])
        h_buf = select_h(hidden, own_meta)
        h_own = swap(h_buf)
        m_f1 = lax.ppermute(meta, 'dp', outer + middle)
        h_f1 = lax.ppermute(hidden, 'dp', outer + middle)
        dy_f1 = lax.ppermute(after(tok_dy, h_f1), 'dp', outer + middle)
        q_buf = select_q(tok_dy, meta)
        q_own = swap(q_buf)
        a_t, b_t = pre(h_own)
        u_t = (a_t * jax.nn.sigmoid(a_t) * b_t).astype(bf16)
        exp_out = jnp.einsum('fr,fd->rd', u_t, wd, preferred_element_type=f32).astype(bf16)
        ep_id = lax.axis_index('ep')
        by_dest = exp_out.reshape(n_ep, slot_cap, d_model)
        pieces = []
        for k in range(n_ep):
            piece = lax.dynamic_index_in_dim(by_dest, ep_id ^ k, 0, keepdims=False)
            if k:
                piece = lax.ppermute(piece, 'ep', [(i, i ^ k) for i in range(n_ep)])
            pieces.append(piece)
        u_t, da_t, db_t = inner_grad(q_own, wd, a_t, b_t)
        grad_hid = (jnp.einsum('fr,fd->rd', da_t, wg_t, preferred_element_type=f32)
                    + jnp.einsum('fr,fd->rd', db_t, wu_t, preferred_element_type=f32)).astype(bf16)
        acc = add_dw(None, u_t, da_t, db_t, h_own, q_own)

        m_f2 = lax.ppermute(m_f1, 'dp', near)
        h_f2 = lax.ppermute(h_f1, 'dp', near)
        dy_f2 = lax.ppermute(dy_f1, 'dp', near)
        h_near = lax.ppermute(h_own, 'dp', near)
        q_near = lax.ppermute(q_own, 'dp', near)
        h_b1 = select_h(h_f1, m_f1)
        q_b1 = select_q(dy_f1, m_f1)
        h_b2 = select_h(h_f2, m_f2)
        q_b2 = select_q(dy_f2, m_f2)
        h_r1 = swap(h_b1)
        q_r1 = swap(q_b1)
        h_r2 = swap(h_b2)
        q_r2 = swap(q_b2)
        hid_back = swap(grad_hid)
        for h, q in ((h_r1, q_r1), (h_r2, q_r2), (h_near, q_near)):
            a_t, b_t = pre(h)
            u_t, da_t, db_t = inner_grad(q, wd, a_t, b_t)
            acc = add_dw(acc, u_t, da_t, db_t, h, q)
        dwg, dwu, dwd = acc

        dy_float = tok_dy.astype(f32)
        sel_one = (pos_one[:, None] == row_ids[None, :]).astype(bf16)
        sel_two = (pos_two[:, None] == row_ids[None, :]).astype(bf16)
        back_one = jnp.where(slot_first >= 0, (exp_first ^ ep_id) * slot_cap + slot_first, -1)
        back_two = jnp.where(slot_second >= 0, (exp_second ^ ep_id) * slot_cap + slot_second, -1)
        out_back = jnp.concatenate(pieces)
        out_one = jnp.dot((back_one[:, None] == row_ids[None, :]).astype(bf16), out_back, preferred_element_type=f32)
        out_two = jnp.dot((back_two[:, None] == row_ids[None, :]).astype(bf16), out_back, preferred_element_type=f32)
        out_tok = (tok_x.astype(f32) + gate_one[:, None] * out_one + gate_two[:, None] * out_two).astype(bf16)
        dgate_one = jnp.sum(dy_float * out_one, axis=-1)
        dgate_two = jnp.sum(dy_float * out_two, axis=-1)
        d_logits = ((dgate_one * gate_one)[:, None] * (pick_one - prob_one)
                    + (dgate_two * gate_two)[:, None] * (pick_two - prob_two)).astype(bf16)
        d_router = jnp.einsum('td,te->ed', hidden, d_logits, preferred_element_type=f32)
        grad_exp = jnp.dot(sel_one + sel_two, hid_back, preferred_element_type=f32)
        grad_h = jnp.einsum('te,de->td', d_logits, router, preferred_element_type=f32) + grad_exp
        d_ln_weight = jnp.sum(grad_h * x_hat, axis=0)
        d_ln_bias = jnp.sum(grad_h, axis=0)
        dx_tok = (dy_float + layer_norm_back(grad_h, x_hat, inv_std, ln_weight)).astype(bf16)
        n_dev = n_dp * n_ep
        parts = jnp.concatenate([d_router, d_ln_weight[None], d_ln_bias[None], jnp.zeros((6, d_model), f32)])
        total = sum_all(parts.reshape(16, n_dev, d_model // n_dev).transpose(1, 0, 2), n_dp, n_ep)
        total = total.transpose(1, 0, 2).reshape(16, d_model)
        d_router, d_ln_weight, d_ln_bias = total[:n_exp].T, total[n_exp], total[n_exp + 1]
        return (out_tok, dx_tok, dwg.T[None], dwu.T[None], dwd[None], d_router, d_ln_weight, d_ln_bias)

    return jax.shard_map(
        local_step, mesh=mesh,
        in_specs=(tok_spec, tok_spec, row_spec, row_spec, tok_spec, row_spec, row_spec,
                  P(), P(), P(), exp_spec, exp_spec, exp_spec),
        out_specs=(tok_spec, tok_spec, exp_spec, exp_spec, exp_spec, P(), P(), P()),
        check_vma=False)
```

```python
import functools

import jax
import jax.numpy as jnp
from jax import lax
from jax.experimental import pallas as pl
from jax.experimental.pallas import tpu as pltpu
from jax.sharding import PartitionSpec as P


LN_EPS = 1e-5
f32 = jnp.float32
bf16 = jnp.bfloat16


def row_mean(value):
    return jnp.mean(value, axis=-1, keepdims=True)


def enter_kernel(x_ref, w_ref, b_ref, pos_ref, hid_ref, buf_ref, mean_ref, inv_ref, h_all, select):
    step = pl.program_id(0)
    n_tok, _ = x_ref.shape
    chunk = n_tok // 8

    @pl.when(step == 0)
    def _():
        def normalize(i, carry):
            rows = pl.ds(pl.multiple_of(i * chunk, chunk), chunk)
            x_float = x_ref[rows, :].astype(f32)
            mean = row_mean(x_float)
            centered = x_float - mean
            inv_std = lax.rsqrt(row_mean(centered * centered) + LN_EPS)
            h_all[rows, :] = (centered * inv_std * w_ref[...].astype(f32) + b_ref[...].astype(f32)).astype(bf16)
            mean_ref[rows, :] = mean
            inv_ref[rows, :] = inv_std
            return carry

        lax.fori_loop(0, n_tok // chunk, normalize, 0)
        row_ids = lax.broadcasted_iota(jnp.int32, select.shape, 0)
        hit = (row_ids == pos_ref[0:1, :]) | (row_ids == pos_ref[1:2, :])
        select[...] = jnp.where(hit, 1.0, 0.0).astype(bf16)

    n_cols = hid_ref.shape[1]
    columns = pl.ds(pl.multiple_of(step * n_cols, n_cols), n_cols)
    part = h_all[:, columns]
    hid_ref[...] = part
    buf_ref[...] = jnp.dot(select[...], part, preferred_element_type=f32).astype(bf16)


def enter(x_rows, weight, bias, pos, n_rows):
    n_tok, d_model = x_rows.shape
    n_cols = d_model // 8
    whole = lambda shape: pl.BlockSpec(shape, lambda j: (0, 0))
    stat = jax.ShapeDtypeStruct((n_tok, 1), f32)
    return pl.pallas_call(
        enter_kernel, grid=(8,),
        in_specs=[whole((n_tok, d_model)), whole((1, d_model)), whole((1, d_model)), whole(pos.shape)],
        out_specs=[pl.BlockSpec((n_tok, n_cols), lambda j: (0, j)), pl.BlockSpec((n_rows, n_cols), lambda j: (0, j)),
                   whole((n_tok, 1)), whole((n_tok, 1))],
        out_shape=[jax.ShapeDtypeStruct((n_tok, d_model), bf16), jax.ShapeDtypeStruct((n_rows, d_model), bf16), stat, stat],
        scratch_shapes=[pltpu.VMEM((n_tok, d_model), bf16), pltpu.VMEM((n_rows, n_tok), bf16)],
        compiler_params=pltpu.CompilerParams(vmem_limit_bytes=48 * 1024 * 1024),
        cost_estimate=pl.CostEstimate(flops=2 * n_rows * n_tok * d_model, bytes_accessed=4 * (n_tok + n_rows) * d_model, transcendentals=n_tok),
    )(x_rows, weight[None], bias[None], pos)


def layer_norm_back(grad_h, x_hat, inv_std, ln_weight):
    scaled = grad_h * ln_weight.astype(f32)
    return inv_std * (scaled - jnp.mean(scaled, axis=-1, keepdims=True)
                      - x_hat * jnp.mean(scaled * x_hat, axis=-1, keepdims=True))


def masked_gate(logits, allowed, choice):
    expert_ids = jnp.arange(logits.shape[-1])
    prob_all = jax.nn.softmax(jnp.where(allowed, logits, -1e30), axis=-1)
    picked = (choice[:, None] == expert_ids[None, :]).astype(f32)
    return jnp.sum(prob_all * picked, axis=-1), prob_all, picked


VMEM_LIMIT = 63 * 1024 * 1024


def grad_kernel(q_ref, wd_ref, a_ref, b_ref, u_ref, da_ref, db_ref):
    du = lax.dot_general(wd_ref[...], q_ref[...], (((1,), (1,)), ((), ())), preferred_element_type=f32)
    pre_gate = a_ref[...]
    pre_up = b_ref[...]
    sig_gate = jax.nn.sigmoid(pre_gate)
    silu_gate = pre_gate * sig_gate
    u_ref[...] = (silu_gate * pre_up).astype(bf16)
    da_ref[...] = (du * pre_up * sig_gate * (1.0 + pre_gate * (1.0 - sig_gate))).astype(bf16)
    db_ref[...] = (du * silu_gate).astype(bf16)


def inner_grad(q, wd, a_t, b_t):
    n_rows, d_model = q.shape
    width = wd.shape[0]
    r_tile = n_rows // 6
    tile = pl.BlockSpec((width, r_tile), lambda j: (0, j))
    return pl.pallas_call(
        grad_kernel,
        grid=(n_rows // r_tile,),
        in_specs=[pl.BlockSpec((r_tile, d_model), lambda j: (j, 0)),
                  pl.BlockSpec((width, d_model), lambda j: (0, 0), pipeline_mode=pl.Buffered(1)),
                  tile, tile],
        out_specs=[tile] * 3,
        out_shape=[jax.ShapeDtypeStruct((width, n_rows), bf16)] * 3,
        compiler_params=pltpu.CompilerParams(vmem_limit_bytes=VMEM_LIMIT),
        cost_estimate=pl.CostEstimate(flops=2 * n_rows * d_model * width, bytes_accessed=4 * n_rows * d_model + 14 * width * n_rows,
                                      transcendentals=2 * n_rows * width),
    )(q, wd, a_t, b_t)


def dw_kernel(first, *refs):
    u_ref, da_ref, db_ref, h_ref, q_ref = refs[:5]
    acc = refs[5:-3]
    outs = refs[-3:]
    for k, (left, right) in enumerate(((da_ref, h_ref), (db_ref, h_ref), (u_ref, q_ref))):
        term = jnp.dot(left[...], right[...], preferred_element_type=f32)
        outs[k][...] = term if first else acc[k][...] + term


def add_dw(acc, u_t, da_t, db_t, h, q):
    width, n_rows = u_t.shape
    d_model = h.shape[1]
    first = acc is None
    acc = [] if first else list(acc)
    d_tile = 512
    whole = pl.BlockSpec((width, n_rows), lambda j: (0, 0), pipeline_mode=pl.Buffered(1))
    rows = pl.BlockSpec((n_rows, d_tile), lambda j: (0, j))
    tile = pl.BlockSpec((width, d_tile), lambda j: (0, j))
    return pl.pallas_call(
        functools.partial(dw_kernel, first),
        grid=(d_model // d_tile,),
        in_specs=[whole] * 3 + [rows] * 2 + [tile] * len(acc),
        out_specs=[tile] * 3,
        out_shape=[jax.ShapeDtypeStruct((width, d_model), f32)] * 3,
        input_output_aliases={5 + k: k for k in range(len(acc))},
        compiler_params=pltpu.CompilerParams(vmem_limit_bytes=VMEM_LIMIT),
        cost_estimate=pl.CostEstimate(flops=6 * n_rows * d_model * width, bytes_accessed=4 * n_rows * d_model + 12 * width * d_model * (1 if first else 2),
                                      transcendentals=0),
    )(u_t, da_t, db_t, h, q, *acc)


def sum_kernel(n_dp, n_ep, x_ref, out_ref, from_ep, from_dp, send_one, recv_one, send_two, recv_two, send_three, recv_three):
    dp, ep = lax.axis_index('dp'), lax.axis_index('ep')
    barrier = pltpu.get_barrier_semaphore()
    peers = [(dp, ep ^ k) for k in range(1, n_ep)] + [(dp ^ k, ep) for k in range(1, n_dp)]
    for device in peers:
        pl.semaphore_signal(barrier, inc=1, device_id=device, device_id_type=pl.DeviceIdType.MESH)
    pl.semaphore_wait(barrier, len(peers))

    def send(src, dst, device, send_sem, recv_sem):
        copy = pltpu.make_async_remote_copy(src_ref=src, dst_ref=dst, send_sem=send_sem, recv_sem=recv_sem,
                                            device_id=device, device_id_type=pl.DeviceIdType.MESH)
        copy.start()
        return copy

    copies = [send(x_ref.at[ep ^ k], from_ep.at[k], (dp, ep ^ k), send_one.at[k], recv_one.at[k]) for k in range(1, n_ep)]
    acc = x_ref[ep]
    for k in range(1, n_ep):
        copies[k - 1].wait_recv()
        acc += from_ep[k]
    from_dp[dp] = acc
    for copy in copies:
        copy.wait_send()
    copies = [send(from_dp.at[dp], from_dp.at[dp], (dp ^ k, ep), send_two.at[k], recv_two.at[k]) for k in range(1, n_dp)]
    for copy in copies:
        copy.wait_recv()
    acc = from_dp[0]
    for k in range(1, n_dp):
        acc += from_dp[k]
    out_ref[ep] = acc
    for copy in copies:
        copy.wait_send()
    copies = [send(out_ref.at[ep], out_ref.at[ep], (dp, ep ^ k), send_three.at[k], recv_three.at[k]) for k in range(1, n_ep)]
    for copy in copies:
        copy.wait_recv()
    for copy in copies:
        copy.wait_send()


def sum_all(x, n_dp, n_ep):
    vmem = pl.BlockSpec(memory_space=pltpu.VMEM)
    dma_ep, dma_dp = pltpu.SemaphoreType.DMA((n_ep,)), pltpu.SemaphoreType.DMA((n_dp,))
    return pl.pallas_call(
        functools.partial(sum_kernel, n_dp, n_ep),
        out_shape=jax.ShapeDtypeStruct(x.shape, f32),
        in_specs=[vmem], out_specs=vmem,
        scratch_shapes=[pltpu.VMEM(x.shape, f32), pltpu.VMEM((n_dp,) + x.shape[1:], f32),
                        dma_ep, dma_ep, dma_dp, dma_dp, dma_ep, dma_ep],
        compiler_params=pltpu.CompilerParams(collective_id=0, has_side_effects=True),
    )(x)


def after(value, *deps):
    return lax.optimization_barrier((value,) + deps)[0]


def solution(mesh):
    n_ep = mesh.shape['ep']
    n_dp = mesh.shape['dp']
    tok_spec = P(('dp', 'ep'), None)
    row_spec = P(('dp', 'ep'))
    exp_spec = P('ep', None, None)
    outer = [(i, i ^ 2) for i in (0, n_dp - 1)]
    middle = [(i, i ^ 2) for i in (1, n_dp - 2)]
    near = [(i, i ^ 1) for i in range(n_dp)]

    def local_step(tok_x, tok_dy, exp_first, exp_second, eligible, slot_first, slot_second,
                   ln_weight, ln_bias, router, w_gate, w_up, w_down):
        n_local, d_model = tok_x.shape
        n_exp = eligible.shape[1]
        slot_cap = 3 * n_local // n_exp
        n_rows = n_exp * slot_cap
        wg_t = w_gate[0].T
        wu_t = w_up[0].T
        wd = w_down[0]

        pos_one = jnp.where(slot_first >= 0, exp_first * slot_cap + slot_first, -1)
        pos_two = jnp.where(slot_second >= 0, exp_second * slot_cap + slot_second, -1)
        hidden, h_buf, mean, inv_std = enter(tok_x, ln_weight, ln_bias, jnp.stack([pos_one, pos_two]), n_rows)
        logits = jnp.dot(hidden, router, preferred_element_type=f32)
        expert_ids = jnp.arange(n_exp)
        allowed = eligible > 0
        gate_one, prob_one, pick_one = masked_gate(logits, allowed, exp_first)
        gate_two, prob_two, pick_two = masked_gate(logits, allowed & (expert_ids[None, :] != exp_first[:, None]), exp_second)
        meta = jnp.stack([pos_one.astype(f32), pos_two.astype(f32), gate_one, gate_two])
        row_ids = jnp.arange(n_rows)

        def masks(meta):
            return [meta[k].astype(jnp.int32)[None, :] == row_ids[:, None] for k in range(2)]

        def select_h(h, meta):
            m1, m2 = masks(meta)
            return jnp.dot((m1 | m2).astype(bf16), h, preferred_element_type=f32).astype(bf16)

        def select_q(dy, meta):
            m1, m2 = masks(meta)
            g_row = jnp.sum(jnp.where(m1, meta[2][None, :], 0.0) + jnp.where(m2, meta[3][None, :], 0.0), axis=1)
            return (g_row[:, None] * jnp.dot((m1 | m2).astype(bf16), dy, preferred_element_type=f32)).astype(bf16)

        def swap(buf):
            return lax.all_to_all(buf.reshape(n_ep, slot_cap, d_model), 'ep', 0, 0, tiled=True).reshape(n_rows, d_model)

        def pre(h):
            return (jnp.einsum('fd,rd->fr', wg_t, h, preferred_element_type=f32),
                    jnp.einsum('fd,rd->fr', wu_t, h, preferred_element_type=f32))

        h_own = swap(h_buf)
        m_f1 = lax.ppermute(meta, 'dp', outer + middle)
        h_f1 = lax.ppermute(hidden, 'dp', outer + middle)
        dy_f1 = lax.ppermute(after(tok_dy, h_f1), 'dp', outer + middle)
        q_buf = select_q(tok_dy, meta)
        q_own = swap(q_buf)
        a_t, b_t = pre(h_own)
        u_t = (a_t * jax.nn.sigmoid(a_t) * b_t).astype(bf16)
        exp_out = jnp.einsum('fr,fd->rd', u_t, wd, preferred_element_type=f32).astype(bf16)
        u_t, da_t, db_t = inner_grad(q_own, wd, a_t, b_t)
        grad_hid = (jnp.einsum('fr,fd->rd', da_t, wg_t, preferred_element_type=f32)
                    + jnp.einsum('fr,fd->rd', db_t, wu_t, preferred_element_type=f32)).astype(bf16)
        acc = add_dw(None, u_t, da_t, db_t, h_own, q_own)

        m_f2 = lax.ppermute(m_f1, 'dp', near)
        h_f2 = lax.ppermute(h_f1, 'dp', near)
        dy_f2 = lax.ppermute(dy_f1, 'dp', near)
        h_near = lax.ppermute(h_own, 'dp', near)
        q_near = lax.ppermute(q_own, 'dp', near)
        h_b1 = select_h(h_f1, m_f1)
        q_b1 = select_q(dy_f1, m_f1)
        h_b2 = select_h(h_f2, m_f2)
        q_b2 = select_q(dy_f2, m_f2)
        h_r1 = swap(h_b1)
        q_r1 = swap(q_b1)
        h_r2 = swap(h_b2)
        q_r2 = swap(q_b2)
        out_back = swap(exp_out)
        hid_back = swap(grad_hid)
        for h, q in ((h_r1, q_r1), (h_r2, q_r2), (h_near, q_near)):
            a_t, b_t = pre(h)
            u_t, da_t, db_t = inner_grad(q, wd, a_t, b_t)
            acc = add_dw(acc, u_t, da_t, db_t, h, q)
        dwg, dwu, dwd = acc

        dy_float = tok_dy.astype(f32)
        sel_one = (pos_one[:, None] == row_ids[None, :]).astype(bf16)
        sel_two = (pos_two[:, None] == row_ids[None, :]).astype(bf16)
        out_one = jnp.dot(sel_one, out_back, preferred_element_type=f32)
        out_two = jnp.dot(sel_two, out_back, preferred_element_type=f32)
        out_tok = (tok_x.astype(f32) + gate_one[:, None] * out_one + gate_two[:, None] * out_two).astype(bf16)
        dgate_one = jnp.sum(dy_float * out_one, axis=-1)
        dgate_two = jnp.sum(dy_float * out_two, axis=-1)
        d_logits = ((dgate_one * gate_one)[:, None] * (pick_one - prob_one)
                    + (dgate_two * gate_two)[:, None] * (pick_two - prob_two)).astype(bf16)
        d_router = jnp.einsum('td,te->ed', hidden, d_logits, preferred_element_type=f32)
        grad_exp = jnp.dot(sel_one + sel_two, hid_back, preferred_element_type=f32)
        grad_h = jnp.einsum('te,de->td', d_logits, router, preferred_element_type=f32) + grad_exp
        x_hat = (tok_x.astype(f32) - mean) * inv_std
        d_ln_weight = jnp.sum(grad_h * x_hat, axis=0)
        d_ln_bias = jnp.sum(grad_h, axis=0)
        dx_tok = (dy_float + layer_norm_back(grad_h, x_hat, inv_std, ln_weight)).astype(bf16)
        small = jnp.concatenate([d_router, d_ln_weight[None], d_ln_bias[None], jnp.zeros((6, d_model), f32)])
        total = sum_all(small.reshape(16, n_ep, d_model // n_ep).transpose(1, 0, 2), n_dp, n_ep).transpose(1, 0, 2).reshape(16, d_model)
        d_router, d_ln_weight, d_ln_bias = total[:n_exp].T, total[n_exp], total[n_exp + 1]
        return (out_tok, dx_tok, dwg.T[None], dwu.T[None], dwd[None], d_router, d_ln_weight, d_ln_bias)

    return jax.shard_map(
        local_step, mesh=mesh,
        in_specs=(tok_spec, tok_spec, row_spec, row_spec, tok_spec, row_spec, row_spec,
                  P(), P(), P(), exp_spec, exp_spec, exp_spec),
        out_specs=(tok_spec, tok_spec, exp_spec, exp_spec, exp_spec, P(), P(), P()),
        check_vma=False)
```

```python
import functools

import jax
import jax.numpy as jnp
from jax import lax
from jax.experimental import pallas as pl
from jax.experimental.pallas import tpu as pltpu
from jax.sharding import PartitionSpec as P


LN_EPS = 1e-5
f32 = jnp.float32
bf16 = jnp.bfloat16


def layer_norm(x_rows, ln_weight, ln_bias):
    x_float = x_rows.astype(f32)
    centered = x_float - jnp.mean(x_float, axis=-1, keepdims=True)
    inv_std = lax.rsqrt(jnp.mean(centered * centered, axis=-1, keepdims=True) + LN_EPS)
    x_hat = centered * inv_std
    hidden = (x_hat * ln_weight.astype(f32) + ln_bias.astype(f32)).astype(bf16)
    return hidden, x_hat, inv_std


def layer_norm_back(grad_h, x_hat, inv_std, ln_weight):
    scaled = grad_h * ln_weight.astype(f32)
    return inv_std * (scaled - jnp.mean(scaled, axis=-1, keepdims=True)
                      - x_hat * jnp.mean(scaled * x_hat, axis=-1, keepdims=True))


def masked_gate(logits, allowed, choice):
    expert_ids = jnp.arange(logits.shape[-1])
    prob_all = jax.nn.softmax(jnp.where(allowed, logits, -1e30), axis=-1)
    picked = (choice[:, None] == expert_ids[None, :]).astype(f32)
    return jnp.sum(prob_all * picked, axis=-1), prob_all, picked


VMEM_LIMIT = 63 * 1024 * 1024


def grad_kernel(q_ref, wd_ref, a_ref, b_ref, u_ref, da_ref, db_ref):
    du = lax.dot_general(wd_ref[...], q_ref[...], (((1,), (1,)), ((), ())), preferred_element_type=f32)
    pre_gate = a_ref[...]
    pre_up = b_ref[...]
    sig_gate = jax.nn.sigmoid(pre_gate)
    silu_gate = pre_gate * sig_gate
    u_ref[...] = (silu_gate * pre_up).astype(bf16)
    da_ref[...] = (du * pre_up * sig_gate * (1.0 + pre_gate * (1.0 - sig_gate))).astype(bf16)
    db_ref[...] = (du * silu_gate).astype(bf16)


def inner_grad(q, wd, a_t, b_t):
    n_rows, d_model = q.shape
    width = wd.shape[0]
    r_tile = n_rows // 6
    tile = pl.BlockSpec((width, r_tile), lambda j: (0, j))
    return pl.pallas_call(
        grad_kernel,
        grid=(n_rows // r_tile,),
        in_specs=[pl.BlockSpec((r_tile, d_model), lambda j: (j, 0)),
                  pl.BlockSpec((width, d_model), lambda j: (0, 0), pipeline_mode=pl.Buffered(1)),
                  tile, tile],
        out_specs=[tile] * 3,
        out_shape=[jax.ShapeDtypeStruct((width, n_rows), bf16)] * 3,
        compiler_params=pltpu.CompilerParams(vmem_limit_bytes=VMEM_LIMIT),
        cost_estimate=pl.CostEstimate(flops=2 * n_rows * d_model * width, bytes_accessed=4 * n_rows * d_model + 14 * width * n_rows,
                                      transcendentals=2 * n_rows * width),
    )(q, wd, a_t, b_t)


def dw_kernel(first, *refs):
    u_ref, da_ref, db_ref, h_ref, q_ref = refs[:5]
    acc = refs[5:-3]
    outs = refs[-3:]
    for k, (left, right) in enumerate(((da_ref, h_ref), (db_ref, h_ref), (u_ref, q_ref))):
        term = jnp.dot(left[...], right[...], preferred_element_type=f32)
        outs[k][...] = term if first else acc[k][...] + term


def add_dw(acc, u_t, da_t, db_t, h, q):
    width, n_rows = u_t.shape
    d_model = h.shape[1]
    first = acc is None
    acc = [] if first else list(acc)
    d_tile = 512
    whole = pl.BlockSpec((width, n_rows), lambda j: (0, 0), pipeline_mode=pl.Buffered(1))
    rows = pl.BlockSpec((n_rows, d_tile), lambda j: (0, j))
    tile = pl.BlockSpec((width, d_tile), lambda j: (0, j))
    return pl.pallas_call(
        functools.partial(dw_kernel, first),
        grid=(d_model // d_tile,),
        in_specs=[whole] * 3 + [rows] * 2 + [tile] * len(acc),
        out_specs=[tile] * 3,
        out_shape=[jax.ShapeDtypeStruct((width, d_model), f32)] * 3,
        input_output_aliases={5 + k: k for k in range(len(acc))},
        compiler_params=pltpu.CompilerParams(vmem_limit_bytes=VMEM_LIMIT),
        cost_estimate=pl.CostEstimate(flops=6 * n_rows * d_model * width, bytes_accessed=4 * n_rows * d_model + 12 * width * d_model * (1 if first else 2),
                                      transcendentals=0),
    )(u_t, da_t, db_t, h, q, *acc)


def sum_kernel(n_dp, n_ep, x_ref, out_ref, from_ep, from_dp, send_one, recv_one, send_two, recv_two, send_three, recv_three):
    dp, ep = lax.axis_index('dp'), lax.axis_index('ep')
    barrier = pltpu.get_barrier_semaphore()
    peers = [(dp, ep ^ k) for k in range(1, n_ep)] + [(dp ^ k, ep) for k in range(1, n_dp)]
    for device in peers:
        pl.semaphore_signal(barrier, inc=1, device_id=device, device_id_type=pl.DeviceIdType.MESH)
    pl.semaphore_wait(barrier, len(peers))

    def send(src, dst, device, send_sem, recv_sem):
        copy = pltpu.make_async_remote_copy(src_ref=src, dst_ref=dst, send_sem=send_sem, recv_sem=recv_sem,
                                            device_id=device, device_id_type=pl.DeviceIdType.MESH)
        copy.start()
        return copy

    copies = [send(x_ref.at[ep ^ k], from_ep.at[k], (dp, ep ^ k), send_one.at[k], recv_one.at[k]) for k in range(1, n_ep)]
    acc = x_ref[ep]
    for k in range(1, n_ep):
        copies[k - 1].wait_recv()
        acc += from_ep[k]
    from_dp[dp] = acc
    for copy in copies:
        copy.wait_send()
    copies = [send(from_dp.at[dp], from_dp.at[dp], (dp ^ k, ep), send_two.at[k], recv_two.at[k]) for k in range(1, n_dp)]
    for copy in copies:
        copy.wait_recv()
    acc = from_dp[0]
    for k in range(1, n_dp):
        acc += from_dp[k]
    out_ref[ep] = acc
    for copy in copies:
        copy.wait_send()
    copies = [send(out_ref.at[ep], out_ref.at[ep], (dp, ep ^ k), send_three.at[k], recv_three.at[k]) for k in range(1, n_ep)]
    for copy in copies:
        copy.wait_recv()
    for copy in copies:
        copy.wait_send()


def sum_all(x, n_dp, n_ep):
    vmem = pl.BlockSpec(memory_space=pltpu.VMEM)
    dma_ep, dma_dp = pltpu.SemaphoreType.DMA((n_ep,)), pltpu.SemaphoreType.DMA((n_dp,))
    return pl.pallas_call(
        functools.partial(sum_kernel, n_dp, n_ep),
        out_shape=jax.ShapeDtypeStruct(x.shape, f32),
        in_specs=[vmem], out_specs=vmem,
        scratch_shapes=[pltpu.VMEM(x.shape, f32), pltpu.VMEM((n_dp,) + x.shape[1:], f32),
                        dma_ep, dma_ep, dma_dp, dma_dp, dma_ep, dma_ep],
        compiler_params=pltpu.CompilerParams(collective_id=0, has_side_effects=True),
    )(x)


def after(value, *deps):
    return lax.optimization_barrier((value,) + deps)[0]


def solution(mesh):
    n_ep = mesh.shape['ep']
    n_dp = mesh.shape['dp']
    tok_spec = P(('dp', 'ep'), None)
    row_spec = P(('dp', 'ep'))
    exp_spec = P('ep', None, None)
    outer = [(i, i ^ 2) for i in (0, n_dp - 1)]
    middle = [(i, i ^ 2) for i in (1, n_dp - 2)]
    near = [(i, i ^ 1) for i in range(n_dp)]

    def local_step(tok_x, tok_dy, exp_first, exp_second, eligible, slot_first, slot_second,
                   ln_weight, ln_bias, router, w_gate, w_up, w_down):
        n_local, d_model = tok_x.shape
        n_exp = eligible.shape[1]
        slot_cap = 3 * n_local // n_exp
        n_rows = n_exp * slot_cap
        wg_t = w_gate[0].T
        wu_t = w_up[0].T
        wd = w_down[0]

        hidden, x_hat, inv_std = layer_norm(tok_x, ln_weight, ln_bias)
        logits = jnp.dot(hidden, router, preferred_element_type=f32)
        expert_ids = jnp.arange(n_exp)
        allowed = eligible > 0
        gate_one, prob_one, pick_one = masked_gate(logits, allowed, exp_first)
        gate_two, prob_two, pick_two = masked_gate(logits, allowed & (expert_ids[None, :] != exp_first[:, None]), exp_second)
        pos_one = jnp.where(slot_first >= 0, exp_first * slot_cap + slot_first, -1)
        pos_two = jnp.where(slot_second >= 0, exp_second * slot_cap + slot_second, -1)
        meta = jnp.stack([pos_one.astype(f32), pos_two.astype(f32), gate_one, gate_two])
        row_ids = jnp.arange(n_rows)

        def masks(meta):
            return [meta[k].astype(jnp.int32)[None, :] == row_ids[:, None] for k in range(2)]

        def select_h(h, meta):
            m1, m2 = masks(meta)
            return jnp.dot((m1 | m2).astype(bf16), h, preferred_element_type=f32).astype(bf16)

        def select_q(dy, meta):
            m1, m2 = masks(meta)
            g_row = jnp.sum(jnp.where(m1, meta[2][None, :], 0.0) + jnp.where(m2, meta[3][None, :], 0.0), axis=1)
            return (g_row[:, None] * jnp.dot((m1 | m2).astype(bf16), dy, preferred_element_type=f32)).astype(bf16)

        def swap(buf):
            return lax.all_to_all(buf.reshape(n_ep, slot_cap, d_model), 'ep', 0, 0, tiled=True).reshape(n_rows, d_model)

        def pre(h):
            return (jnp.einsum('fd,rd->fr', wg_t, h, preferred_element_type=f32),
                    jnp.einsum('fd,rd->fr', wu_t, h, preferred_element_type=f32))

        own_meta = jnp.stack([pos_one.astype(f32), pos_two.astype(f32)])
        h_buf = select_h(hidden, own_meta)
        h_own = swap(h_buf)
        m_f1 = lax.ppermute(meta, 'dp', outer + middle)
        h_f1 = lax.ppermute(hidden, 'dp', outer + middle)
        dy_f1 = lax.ppermute(after(tok_dy, h_f1), 'dp', outer + middle)
        q_buf = select_q(tok_dy, meta)
        q_own = swap(q_buf)
        a_t, b_t = pre(h_own)
        u_t = (a_t * jax.nn.sigmoid(a_t) * b_t).astype(bf16)
        exp_out = jnp.einsum('fr,fd->rd', u_t, wd, preferred_element_type=f32).astype(bf16)
        ep_id = lax.axis_index('ep')
        by_dest = exp_out.reshape(n_ep, slot_cap, d_model)
        pieces = []
        for k in range(n_ep):
            piece = lax.dynamic_index_in_dim(by_dest, ep_id ^ k, 0, keepdims=False)
            if k:
                piece = lax.ppermute(piece, 'ep', [(i, i ^ k) for i in range(n_ep)])
            pieces.append(piece)
        u_t, da_t, db_t = inner_grad(q_own, wd, a_t, b_t)
        grad_hid = (jnp.einsum('fr,fd->rd', da_t, wg_t, preferred_element_type=f32)
                    + jnp.einsum('fr,fd->rd', db_t, wu_t, preferred_element_type=f32)).astype(bf16)
        acc = add_dw(None, u_t, da_t, db_t, h_own, q_own)

        m_f2 = lax.ppermute(m_f1, 'dp', near)
        h_f2 = lax.ppermute(h_f1, 'dp', near)
        dy_f2 = lax.ppermute(dy_f1, 'dp', near)
        h_near = lax.ppermute(h_own, 'dp', near)
        q_near = lax.ppermute(q_own, 'dp', near)
        h_b1 = select_h(h_f1, m_f1)
        q_b1 = select_q(dy_f1, m_f1)
        h_b2 = select_h(h_f2, m_f2)
        q_b2 = select_q(dy_f2, m_f2)
        h_r1 = swap(h_b1)
        q_r1 = swap(q_b1)
        h_r2 = swap(h_b2)
        q_r2 = swap(q_b2)
        hid_back = swap(grad_hid)
        for h, q in ((h_r1, q_r1), (h_r2, q_r2), (h_near, q_near)):
            a_t, b_t = pre(h)
            u_t, da_t, db_t = inner_grad(q, wd, a_t, b_t)
            acc = add_dw(acc, u_t, da_t, db_t, h, q)
        dwg, dwu, dwd = acc

        dy_float = tok_dy.astype(f32)
        sel_one = (pos_one[:, None] == row_ids[None, :]).astype(bf16)
        sel_two = (pos_two[:, None] == row_ids[None, :]).astype(bf16)
        back_one = jnp.where(slot_first >= 0, (after(exp_first, a_t) ^ ep_id) * slot_cap + slot_first, -1)
        back_two = jnp.where(slot_second >= 0, (after(exp_second, a_t) ^ ep_id) * slot_cap + slot_second, -1)
        out_back = jnp.concatenate(pieces)
        out_one = jnp.dot((back_one[:, None] == row_ids[None, :]).astype(bf16), out_back, preferred_element_type=f32)
        out_two = jnp.dot((back_two[:, None] == row_ids[None, :]).astype(bf16), out_back, preferred_element_type=f32)
        out_tok = (tok_x.astype(f32) + gate_one[:, None] * out_one + gate_two[:, None] * out_two).astype(bf16)
        dgate_one = jnp.sum(dy_float * out_one, axis=-1)
        dgate_two = jnp.sum(dy_float * out_two, axis=-1)
        d_logits = ((dgate_one * gate_one)[:, None] * (pick_one - prob_one)
                    + (dgate_two * gate_two)[:, None] * (pick_two - prob_two)).astype(bf16)
        d_router = jnp.einsum('td,te->ed', hidden, d_logits, preferred_element_type=f32)
        grad_exp = jnp.dot(sel_one + sel_two, hid_back, preferred_element_type=f32)
        grad_h = jnp.einsum('te,de->td', d_logits, router, preferred_element_type=f32) + grad_exp
        d_ln_weight = jnp.sum(grad_h * x_hat, axis=0)
        d_ln_bias = jnp.sum(grad_h, axis=0)
        dx_tok = (dy_float + layer_norm_back(grad_h, x_hat, inv_std, ln_weight)).astype(bf16)
        small = jnp.concatenate([d_router, d_ln_weight[None], d_ln_bias[None], jnp.zeros((6, d_model), f32)])
        total = sum_all(small.reshape(16, n_ep, d_model // n_ep).transpose(1, 0, 2), n_dp, n_ep).transpose(1, 0, 2).reshape(16, d_model)
        d_router, d_ln_weight, d_ln_bias = total[:n_exp].T, total[n_exp], total[n_exp + 1]
        return (out_tok, dx_tok, dwg.T[None], dwu.T[None], dwd[None], d_router, d_ln_weight, d_ln_bias)

    return jax.shard_map(
        local_step, mesh=mesh,
        in_specs=(tok_spec, tok_spec, row_spec, row_spec, tok_spec, row_spec, row_spec,
                  P(), P(), P(), exp_spec, exp_spec, exp_spec),
        out_specs=(tok_spec, tok_spec, exp_spec, exp_spec, exp_spec, P(), P(), P()),
        check_vma=False)
```

```python
import functools

import jax
import jax.numpy as jnp
from jax import lax
from jax.experimental import pallas as pl
from jax.experimental.pallas import tpu as pltpu
from jax.sharding import PartitionSpec as P


LN_EPS = 1e-5
f32 = jnp.float32
bf16 = jnp.bfloat16


def layer_norm(x_rows, ln_weight, ln_bias):
    x_float = x_rows.astype(f32)
    centered = x_float - jnp.mean(x_float, axis=-1, keepdims=True)
    inv_std = lax.rsqrt(jnp.mean(centered * centered, axis=-1, keepdims=True) + LN_EPS)
    x_hat = centered * inv_std
    hidden = (x_hat * ln_weight.astype(f32) + ln_bias.astype(f32)).astype(bf16)
    return hidden, x_hat, inv_std


def layer_norm_back(grad_h, x_hat, inv_std, ln_weight):
    scaled = grad_h * ln_weight.astype(f32)
    return inv_std * (scaled - jnp.mean(scaled, axis=-1, keepdims=True)
                      - x_hat * jnp.mean(scaled * x_hat, axis=-1, keepdims=True))


def masked_gate(logits, allowed, choice):
    expert_ids = jnp.arange(logits.shape[-1])
    prob_all = jax.nn.softmax(jnp.where(allowed, logits, -1e30), axis=-1)
    picked = (choice[:, None] == expert_ids[None, :]).astype(f32)
    return jnp.sum(prob_all * picked, axis=-1), prob_all, picked


VMEM_LIMIT = 63 * 1024 * 1024


def grad_kernel(q_ref, wd_ref, a_ref, b_ref, u_ref, da_ref, db_ref):
    du = lax.dot_general(wd_ref[...], q_ref[...], (((1,), (1,)), ((), ())), preferred_element_type=f32)
    pre_gate = a_ref[...]
    pre_up = b_ref[...]
    sig_gate = jax.nn.sigmoid(pre_gate)
    silu_gate = pre_gate * sig_gate
    u_ref[...] = (silu_gate * pre_up).astype(bf16)
    da_ref[...] = (du * pre_up * sig_gate * (1.0 + pre_gate * (1.0 - sig_gate))).astype(bf16)
    db_ref[...] = (du * silu_gate).astype(bf16)


def inner_grad(q, wd, a_t, b_t):
    n_rows, d_model = q.shape
    width = wd.shape[0]
    r_tile = n_rows // 6
    tile = pl.BlockSpec((width, r_tile), lambda j: (0, j))
    return pl.pallas_call(
        grad_kernel,
        grid=(n_rows // r_tile,),
        in_specs=[pl.BlockSpec((r_tile, d_model), lambda j: (j, 0)),
                  pl.BlockSpec((width, d_model), lambda j: (0, 0), pipeline_mode=pl.Buffered(1)),
                  tile, tile],
        out_specs=[tile] * 3,
        out_shape=[jax.ShapeDtypeStruct((width, n_rows), bf16)] * 3,
        compiler_params=pltpu.CompilerParams(vmem_limit_bytes=VMEM_LIMIT),
        cost_estimate=pl.CostEstimate(flops=2 * n_rows * d_model * width, bytes_accessed=4 * n_rows * d_model + 14 * width * n_rows,
                                      transcendentals=2 * n_rows * width),
    )(q, wd, a_t, b_t)


def dw_kernel(first, *refs):
    u_ref, da_ref, db_ref, h_ref, q_ref = refs[:5]
    acc = refs[5:-3]
    outs = refs[-3:]
    for k, (left, right) in enumerate(((da_ref, h_ref), (db_ref, h_ref), (u_ref, q_ref))):
        term = jnp.dot(left[...], right[...], preferred_element_type=f32)
        outs[k][...] = term if first else acc[k][...] + term


def add_dw(acc, u_t, da_t, db_t, h, q):
    width, n_rows = u_t.shape
    d_model = h.shape[1]
    first = acc is None
    acc = [] if first else list(acc)
    d_tile = 512
    whole = pl.BlockSpec((width, n_rows), lambda j: (0, 0), pipeline_mode=pl.Buffered(1))
    rows = pl.BlockSpec((n_rows, d_tile), lambda j: (0, j))
    tile = pl.BlockSpec((width, d_tile), lambda j: (0, j))
    return pl.pallas_call(
        functools.partial(dw_kernel, first),
        grid=(d_model // d_tile,),
        in_specs=[whole] * 3 + [rows] * 2 + [tile] * len(acc),
        out_specs=[tile] * 3,
        out_shape=[jax.ShapeDtypeStruct((width, d_model), f32)] * 3,
        input_output_aliases={5 + k: k for k in range(len(acc))},
        compiler_params=pltpu.CompilerParams(vmem_limit_bytes=VMEM_LIMIT),
        cost_estimate=pl.CostEstimate(flops=6 * n_rows * d_model * width, bytes_accessed=4 * n_rows * d_model + 12 * width * d_model * (1 if first else 2),
                                      transcendentals=0),
    )(u_t, da_t, db_t, h, q, *acc)


def sum_kernel(n_dp, n_ep, x_ref, out_ref, from_ep, from_dp, send_one, recv_one, send_two, recv_two, send_three, recv_three):
    dp, ep = lax.axis_index('dp'), lax.axis_index('ep')
    barrier = pltpu.get_barrier_semaphore()
    peers = [(dp, ep ^ k) for k in range(1, n_ep)] + [(dp ^ k, ep) for k in range(1, n_dp)]
    for device in peers:
        pl.semaphore_signal(barrier, inc=1, device_id=device, device_id_type=pl.DeviceIdType.MESH)
    pl.semaphore_wait(barrier, len(peers))

    def send(src, dst, device, send_sem, recv_sem):
        copy = pltpu.make_async_remote_copy(src_ref=src, dst_ref=dst, send_sem=send_sem, recv_sem=recv_sem,
                                            device_id=device, device_id_type=pl.DeviceIdType.MESH)
        copy.start()
        return copy

    copies = [send(x_ref.at[ep ^ k], from_ep.at[k], (dp, ep ^ k), send_one.at[k], recv_one.at[k]) for k in range(1, n_ep)]
    acc = x_ref[ep]
    for k in range(1, n_ep):
        copies[k - 1].wait_recv()
        acc += from_ep[k]
    from_dp[dp] = acc
    for copy in copies:
        copy.wait_send()
    copies = [send(from_dp.at[dp], from_dp.at[dp], (dp ^ k, ep), send_two.at[k], recv_two.at[k]) for k in range(1, n_dp)]
    for copy in copies:
        copy.wait_recv()
    acc = from_dp[0]
    for k in range(1, n_dp):
        acc += from_dp[k]
    out_ref[ep] = acc
    for copy in copies:
        copy.wait_send()
    copies = [send(out_ref.at[ep], out_ref.at[ep], (dp, ep ^ k), send_three.at[k], recv_three.at[k]) for k in range(1, n_ep)]
    for copy in copies:
        copy.wait_recv()
    for copy in copies:
        copy.wait_send()


def sum_all(x, n_dp, n_ep):
    vmem = pl.BlockSpec(memory_space=pltpu.VMEM)
    dma_ep, dma_dp = pltpu.SemaphoreType.DMA((n_ep,)), pltpu.SemaphoreType.DMA((n_dp,))
    return pl.pallas_call(
        functools.partial(sum_kernel, n_dp, n_ep),
        out_shape=jax.ShapeDtypeStruct(x.shape, f32),
        in_specs=[vmem], out_specs=vmem,
        scratch_shapes=[pltpu.VMEM(x.shape, f32), pltpu.VMEM((n_dp,) + x.shape[1:], f32),
                        dma_ep, dma_ep, dma_dp, dma_dp, dma_ep, dma_ep],
        compiler_params=pltpu.CompilerParams(collective_id=0, has_side_effects=True),
    )(x)


def after(value, *deps):
    return lax.optimization_barrier((value,) + deps)[0]


def solution(mesh):
    n_ep = mesh.shape['ep']
    n_dp = mesh.shape['dp']
    tok_spec = P(('dp', 'ep'), None)
    row_spec = P(('dp', 'ep'))
    exp_spec = P('ep', None, None)
    outer = [(i, i ^ 2) for i in (0, n_dp - 1)]
    middle = [(i, i ^ 2) for i in (1, n_dp - 2)]
    near = [(i, i ^ 1) for i in range(n_dp)]

    def local_step(tok_x, tok_dy, exp_first, exp_second, eligible, slot_first, slot_second,
                   ln_weight, ln_bias, router, w_gate, w_up, w_down):
        n_local, d_model = tok_x.shape
        n_exp = eligible.shape[1]
        slot_cap = 3 * n_local // n_exp
        n_rows = n_exp * slot_cap
        wg_t = w_gate[0].T
        wu_t = w_up[0].T
        wd = w_down[0]

        hidden, x_hat, inv_std = layer_norm(tok_x, ln_weight, ln_bias)
        logits = jnp.dot(hidden, router, preferred_element_type=f32)
        expert_ids = jnp.arange(n_exp)
        allowed = eligible > 0
        gate_one, prob_one, pick_one = masked_gate(logits, allowed, exp_first)
        gate_two, prob_two, pick_two = masked_gate(logits, allowed & (expert_ids[None, :] != exp_first[:, None]), exp_second)
        pos_one = jnp.where(slot_first >= 0, exp_first * slot_cap + slot_first, -1)
        pos_two = jnp.where(slot_second >= 0, exp_second * slot_cap + slot_second, -1)
        meta = jnp.stack([pos_one.astype(f32), pos_two.astype(f32), gate_one, gate_two])
        row_ids = jnp.arange(n_rows)

        def masks(meta):
            return [meta[k].astype(jnp.int32)[None, :] == row_ids[:, None] for k in range(2)]

        def select_h(h, meta):
            m1, m2 = masks(meta)
            return jnp.dot((m1 | m2).astype(bf16), h, preferred_element_type=f32).astype(bf16)

        def select_q(dy, meta):
            m1, m2 = masks(meta)
            g_row = jnp.sum(jnp.where(m1, meta[2][None, :], 0.0) + jnp.where(m2, meta[3][None, :], 0.0), axis=1)
            return (g_row[:, None] * jnp.dot((m1 | m2).astype(bf16), dy, preferred_element_type=f32)).astype(bf16)

        def swap(buf):
            return lax.all_to_all(buf.reshape(n_ep, slot_cap, d_model), 'ep', 0, 0, tiled=True).reshape(n_rows, d_model)

        def pre(h):
            return (jnp.einsum('fd,rd->fr', wg_t, h, preferred_element_type=f32),
                    jnp.einsum('fd,rd->fr', wu_t, h, preferred_element_type=f32))

        own_meta = jnp.stack([pos_one.astype(f32), pos_two.astype(f32)])
        h_buf = select_h(hidden, own_meta)
        h_own = swap(h_buf)
        m_f1 = lax.ppermute(meta, 'dp', outer + middle)
        h_f1 = lax.ppermute(hidden, 'dp', outer + middle)
        dy_f1 = lax.ppermute(after(tok_dy, h_f1), 'dp', outer + middle)
        q_buf = select_q(tok_dy, meta)
        ep_id = lax.axis_index('ep')
        by_dest = q_buf.reshape(n_ep, slot_cap, d_model)
        q_own = jnp.zeros_like(by_dest)
        for k in range(n_ep):
            piece = lax.dynamic_index_in_dim(by_dest, ep_id ^ k, 0, keepdims=False)
            if k:
                piece = lax.ppermute(piece, 'ep', [(i, i ^ k) for i in range(n_ep)])
            q_own = lax.dynamic_update_index_in_dim(q_own, piece, ep_id ^ k, 0)
        q_own = q_own.reshape(n_rows, d_model)
        a_t, b_t = pre(h_own)
        u_t = (a_t * jax.nn.sigmoid(a_t) * b_t).astype(bf16)
        exp_out = jnp.einsum('fr,fd->rd', u_t, wd, preferred_element_type=f32).astype(bf16)
        by_dest = exp_out.reshape(n_ep, slot_cap, d_model)
        pieces = []
        for k in range(n_ep):
            piece = lax.dynamic_index_in_dim(by_dest, ep_id ^ k, 0, keepdims=False)
            if k:
                piece = lax.ppermute(piece, 'ep', [(i, i ^ k) for i in range(n_ep)])
            pieces.append(piece)
        u_t, da_t, db_t = inner_grad(q_own, wd, a_t, b_t)
        grad_hid = (jnp.einsum('fr,fd->rd', da_t, wg_t, preferred_element_type=f32)
                    + jnp.einsum('fr,fd->rd', db_t, wu_t, preferred_element_type=f32)).astype(bf16)
        acc = add_dw(None, u_t, da_t, db_t, h_own, q_own)

        m_f2 = lax.ppermute(m_f1, 'dp', near)
        h_f2 = lax.ppermute(h_f1, 'dp', near)
        dy_f2 = lax.ppermute(dy_f1, 'dp', near)
        h_near = lax.ppermute(h_own, 'dp', near)
        q_near = lax.ppermute(q_own, 'dp', near)
        h_b1 = select_h(h_f1, m_f1)
        q_b1 = select_q(dy_f1, m_f1)
        h_b2 = select_h(h_f2, m_f2)
        q_b2 = select_q(dy_f2, m_f2)
        h_r1 = swap(h_b1)
        q_r1 = swap(q_b1)
        h_r2 = swap(h_b2)
        q_r2 = swap(q_b2)
        hid_back = swap(grad_hid)
        for h, q in ((h_r1, q_r1), (h_r2, q_r2), (h_near, q_near)):
            a_t, b_t = pre(h)
            u_t, da_t, db_t = inner_grad(q, wd, a_t, b_t)
            acc = add_dw(acc, u_t, da_t, db_t, h, q)
        dwg, dwu, dwd = acc

        dy_float = tok_dy.astype(f32)
        sel_one = (pos_one[:, None] == row_ids[None, :]).astype(bf16)
        sel_two = (pos_two[:, None] == row_ids[None, :]).astype(bf16)
        back_one = jnp.where(slot_first >= 0, (after(exp_first, a_t) ^ ep_id) * slot_cap + slot_first, -1)
        back_two = jnp.where(slot_second >= 0, (after(exp_second, a_t) ^ ep_id) * slot_cap + slot_second, -1)
        out_back = jnp.concatenate(pieces)
        out_one = jnp.dot((back_one[:, None] == row_ids[None, :]).astype(bf16), out_back, preferred_element_type=f32)
        out_two = jnp.dot((back_two[:, None] == row_ids[None, :]).astype(bf16), out_back, preferred_element_type=f32)
        out_tok = (tok_x.astype(f32) + gate_one[:, None] * out_one + gate_two[:, None] * out_two).astype(bf16)
        dgate_one = jnp.sum(dy_float * out_one, axis=-1)
        dgate_two = jnp.sum(dy_float * out_two, axis=-1)
        d_logits = ((dgate_one * gate_one)[:, None] * (pick_one - prob_one)
                    + (dgate_two * gate_two)[:, None] * (pick_two - prob_two)).astype(bf16)
        d_router = jnp.einsum('td,te->ed', hidden, d_logits, preferred_element_type=f32)
        grad_exp = jnp.dot(sel_one + sel_two, hid_back, preferred_element_type=f32)
        grad_h = jnp.einsum('te,de->td', d_logits, router, preferred_element_type=f32) + grad_exp
        d_ln_weight = jnp.sum(grad_h * x_hat, axis=0)
        d_ln_bias = jnp.sum(grad_h, axis=0)
        dx_tok = (dy_float + layer_norm_back(grad_h, x_hat, inv_std, ln_weight)).astype(bf16)
        small = jnp.concatenate([d_router, d_ln_weight[None], d_ln_bias[None], jnp.zeros((6, d_model), f32)])
        total = sum_all(small.reshape(16, n_ep, d_model // n_ep).transpose(1, 0, 2), n_dp, n_ep).transpose(1, 0, 2).reshape(16, d_model)
        d_router, d_ln_weight, d_ln_bias = total[:n_exp].T, total[n_exp], total[n_exp + 1]
        return (out_tok, dx_tok, dwg.T[None], dwu.T[None], dwd[None], d_router, d_ln_weight, d_ln_bias)

    return jax.shard_map(
        local_step, mesh=mesh,
        in_specs=(tok_spec, tok_spec, row_spec, row_spec, tok_spec, row_spec, row_spec,
                  P(), P(), P(), exp_spec, exp_spec, exp_spec),
        out_specs=(tok_spec, tok_spec, exp_spec, exp_spec, exp_spec, P(), P(), P()),
        check_vma=False)
```
